128 devices in a mesh: ta: 64 (over y, x, z), gz: 2 (over core).
Axes of the slice: x: 4, y: 4, z: 4, core: 2. Of those that a mesh axis runs over, the one named last changes fastest.
Arguments:
- propagator: float32 [2, 12, 12, 64, 13824], P(None, None, None, 'ta', 'gz'), may hold values from -6 to 6
- backward: float32 [2, 12, 12, 64, 13824], P(None, None, None, 'ta', 'gz'), may hold values from -6 to 6
- sink_time: int32 [1], replicated, may hold values from 0 to 63
- source_position: int32 [3], replicated, may hold values from 0 to 23
- momenta: int32 [27, 3], replicated, may hold values from -3 to 3
- gamma_table: int32 [16], replicated, may hold values from 0 to 15, each once
Outputs:
- correlator: float32 [2, 64, 16, 27], P(None, 'ta', 'gz')
The draws below stay inside these ranges and needn't reach their ends.
Inputs may be any that keep to these rules, and one draw needn't show every extreme that they name: `gamma_table`: each of 0 to 15 appears exactly once.
All inputs are finite; a program needn't handle non-finite values.
Results may differ from the reference program's by a relative error of at most 0.00007.
Values sent between devices are 32-bit elements; how exact they have to be, the bound alone decides.
No kernel may reach another device: no remote copies, remote signals or barrier semaphores. Data moves between devices by JAX's collectives and lax.ppermute only.
A program may use at most 192 MiB of HBM per device.

```python
import math
import jax
import jax.numpy as jnp
import numpy as np
from jax import lax

L = 24
NG = 16
NP = 27
T_SIZE = 64
V3 = 13824


def place_ends(drawn, stream_key, smallest, largest):
    shape = drawn.shape
    place = [jax.random.randint(jax.random.fold_in(stream_key, axis), (), 0, shape[axis]) for axis in range(len(shape))]
    drawn = drawn.at[tuple(place)].set(smallest)
    longest = shape.index(max(shape))
    place[longest] = (place[longest] + 1) % shape[longest]
    return drawn.at[tuple(place)].set(largest)


def steps_of(rng, extent, cuts, low, top_value):
    loudness, own = 1.0, jax.random.fold_in(rng, 6)
    for position, shards_of in cuts:
        heights = jnp.exp(jax.random.uniform(jax.random.fold_in(own, position), (shards_of,), jnp.float32, low / len(cuts), top_value / len(cuts)))
        loudness = loudness * jnp.repeat(heights, extent[position] // shards_of).reshape([-1 if axis == position else 1 for axis in range(len(extent))])
    return loudness


def scatter_about(own_key, shape, scale, most, shards=(), kind=jnp.bfloat16):
    gain = steps_of(own_key, shape, shards, -0.22, 0.18) if shards else 1.0
    values = jax.random.normal(own_key, shape, jnp.float32) * scale * gain
    return jnp.minimum(jnp.maximum(values, -most), most).astype(kind)


def setup_inputs(seed: int = 0) -> dict:
    seeds = jax.random.split(jax.random.key(seed), 7)
    return {
        "propagator": scatter_about(seeds[0], (2, 12, 12, T_SIZE, V3), 1.0, 6.0, ((3, 64), (4, 2)), jnp.float32),
        "backward": scatter_about(seeds[1], (2, 12, 12, T_SIZE, V3), 1.0, 6.0, ((3, 64), (4, 2)), jnp.float32),
        "sink_time": jax.random.randint(seeds[2], (1,), 0, T_SIZE).astype(jnp.int32),
        "source_position": jax.random.randint(seeds[3], (3,), 0, L).astype(jnp.int32),
        "momenta": place_ends(jax.random.randint(seeds[4], (NP, 3), -3, 4), jax.random.fold_in(seeds[4], 1), -3, 3).astype(jnp.int32),
        "gamma_table": jax.random.permutation(seeds[5], NG).astype(jnp.int32),
    }


def gamma_tables():
    paulis = [np.eye(2), np.array([[0.0, 1.0], [1.0, 0.0]]), np.array([[0.0, -1j], [1j, 0.0]]), np.array([[1.0, 0.0], [0.0, -1.0]])]
    matrices = np.stack([np.kron(paulis[number // 4], paulis[number % 4]) for number in range(16)])
    return np.stack([matrices.real, matrices.imag]).astype(np.float32)

def complex_product(einsum_form, left_term, right_term):

    def product(first_op, second_op):
        return jnp.einsum(einsum_form, first_op, second_op, precision=lax.Precision.HIGHEST)
    real_part = product(left_term[0], right_term[0]) - product(left_term[1], right_term[1])
    imag_part = product(left_term[0], right_term[1]) + product(left_term[1], right_term[0])
    return jnp.stack([real_part, imag_part])

def complex_reduce(left_term, right_term, reduce_axis):
    real_part = lax.optimization_barrier(jnp.sum(left_term[0] * right_term[0] - left_term[1] * right_term[1], axis=reduce_axis))
    imag_part = lax.optimization_barrier(jnp.sum(left_term[0] * right_term[1] + left_term[1] * right_term[0], axis=reduce_axis))
    return jnp.stack([real_part, imag_part])

def conjugate(values):
    return jnp.stack([values[0], -values[1]])

def source_field(sink_slice):
    return 0.125 * complex_reduce(sink_slice[:, :, None, :, :], sink_slice[:, None, :, :, :], 2)

def phase_table(site_index, source_position, momenta):
    zplane = site_index // (L * L)
    xline = site_index // L % L
    yline = site_index % L
    wave = momenta[:, 0:1] * (xline[None, :] - source_position[0]) + momenta[:, 1:2] * (yline[None, :] - source_position[1]) + momenta[:, 2:3] * (zplane[None, :] - source_position[2])
    wave = jnp.mod(wave, L)
    angle_value = wave.astype(jnp.float32) * (2.0 * math.pi / L)
    return jnp.stack([jnp.cos(angle_value), -jnp.sin(angle_value)])

def slice_correlator(forward, back_field, sink_field, phases, gammas):
    site_count = forward.shape[-1]
    bound = complex_reduce(back_field[:, :, :, None, :], sink_field[:, None, :, :, :], 1)
    forward_split = forward.reshape(2, 4, 36, site_count)
    bound_split = conjugate(bound).reshape(2, 4, 36, site_count)
    spin_block = complex_reduce(forward_split[:, :, None, :, :], bound_split[:, None, :, :, :], 2)
    gamma_flat = jnp.transpose(gammas, (0, 1, 3, 2)).reshape(2, 16, 16)
    currents = complex_product('gb,bs->gs', gamma_flat, spin_block.reshape(2, 16, site_count))
    scale_factor = 1.0 / (72.0 * math.sqrt(L * L * L))
    return scale_factor * complex_product('gs,ps->gp', currents, phases)

def select_currents(gamma_table, values):
    onehot = (gamma_table[:, None] == jnp.arange(NG, dtype=jnp.int32)[None, :]).astype(jnp.float32)
    return jnp.einsum('cg,xgp->xcp', onehot, values, precision=lax.Precision.HIGHEST)

def reference(propagator, backward, sink_time, source_position, momenta, gamma_table):
    gammas = jnp.asarray(gamma_tables())
    sink_slice = lax.dynamic_index_in_dim(propagator, sink_time[0], 3, keepdims=False)
    sink_field = source_field(sink_slice)
    phases = phase_table(jnp.arange(L * L * L, dtype=jnp.int32), source_position, momenta)

    def one_slice(slice_index):
        forward = lax.dynamic_index_in_dim(propagator, slice_index, 3, keepdims=False)
        back_field = lax.dynamic_index_in_dim(backward, slice_index, 3, keepdims=False)
        return select_currents(gamma_table, slice_correlator(forward, back_field, sink_field, phases, gammas))
    stacked = lax.map(one_slice, jnp.arange(T_SIZE, dtype=jnp.int32))
    return jnp.transpose(stacked, (1, 0, 2, 3))
```

```python
import math

import jax
import jax.numpy as jnp
import numpy as np
from jax import lax
from jax.experimental import pallas as pl
from jax.experimental.pallas import tpu as pltpu
from jax.sharding import PartitionSpec as P

L = 24
NG = 16
NP = 27
ROWS = 54
A_START = (0, 14, 28, 42)
B_START = (8, 22, 36, 48)
GROUP = 560
F32 = jnp.float32
BF16 = jnp.bfloat16


def pair_index(m, n):
    m, n = min(m, n), max(m, n)
    return m * 12 - m * (m - 1) // 2 + (n - m)


def gamma_weights():
    paulis = [
        np.eye(2),
        np.array([[0.0, 1.0], [1.0, 0.0]]),
        np.array([[0.0, -1j], [1j, 0.0]]),
        np.array([[1.0, 0.0], [0.0, -1.0]]),
    ]
    matrices = np.stack([np.kron(paulis[number // 4], paulis[number % 4]) for number in range(16)])
    flat = matrices.reshape(16, 16) / (72.0 * math.sqrt(L * L * L))
    top = np.concatenate([flat.real, -flat.imag], axis=1)
    low = np.concatenate([flat.imag, flat.real], axis=1)
    return np.stack([top, low]).astype(np.float32)


def block_copy(field, start, rows, buf, sem):
    return pltpu.make_async_copy(
        field.at[:, pl.ds(start, rows), 0, :], buf.at[:, pl.ds(0, rows), :], sem
    )


def source_block(buf, sums, write):
    for e in range(144):
        sums[e] = buf[e] + buf[144 + e]
    for mt in range(0, 12, 3):
        for nt in range(mt, 12, 3):
            pairs = [(m, n) for m in range(mt, mt + 3) for n in range(nt, nt + 3) if m <= n]
            acc = {}
            for k in range(12):
                rows = sorted({m for m, _ in pairs} | {n for _, n in pairs})
                re = {m: buf[m * 12 + k] for m in rows}
                im = {m: buf[144 + m * 12 + k] for m in rows}
                su = {m: sums[m * 12 + k] for m in rows}
                for m, n in pairs:
                    new = (re[m] * re[n], im[m] * im[n], su[m] * su[n])
                    acc[m, n] = new if k == 0 else tuple(a + b for a, b in zip(acc[m, n], new))
            for m, n in pairs:
                p1, p2, p3 = acc[m, n]
                write(pair_index(m, n), 0.125 * (p1 - p2), 0.125 * (p3 - p1 - p2))


def source_kernel(owner_ref, field, out_ref, buf_a, buf_b, sums, sems):
    c = pl.program_id(0)
    mine = owner_ref[0] == 1

    def copies(q):
        return [
            block_copy(field, A_START[q], 8, buf_a.at[q], sems.at[q, 0]),
            block_copy(field, B_START[q], 6, buf_b.at[q], sems.at[q, 1]),
        ]

    @pl.when(mine & (c == 0))
    def _():
        for q in range(4):
            for copy in copies(q):
                copy.start()

    @pl.when(mine)
    def _():
        for q in range(4):

            @pl.when(c == q)
            def _():
                for copy in copies(q):
                    copy.wait()

        def write_a(u, re, im):
            for e, v in ((u, re), (78 + u, im)):
                out_ref[0, e // 39, e % 39 * 8 : e % 39 * 8 + 8, :] = v

        def write_b(u, re, im):
            for e, v in ((u, re), (78 + u, im)):
                out_ref[0, e // 39, 320 + e % 39 * 6 : 320 + e % 39 * 6 + 6, :] = v[:6]

        source_block(buf_a.at[c], sums, write_a)
        source_block(buf_b.at[c], sums, write_b)

    @pl.when(jnp.logical_not(mine))
    def _():
        out_ref[...] = jnp.zeros_like(out_ref)


def source(owner, field):
    return pl.pallas_call(
        source_kernel,
        grid_spec=pltpu.PrefetchScalarGridSpec(
            num_scalar_prefetch=1,
            grid=(4,),
            in_specs=[pl.BlockSpec(memory_space=pl.ANY)],
            out_specs=pl.BlockSpec((1, 4, GROUP, 128), lambda c, s: (c, 0, 0, 0)),
            scratch_shapes=[
                pltpu.VMEM((4, 288, 8, 128), F32),
                pltpu.VMEM((4, 288, 8, 128), F32),
                pltpu.VMEM((144, 8, 128), F32),
                pltpu.SemaphoreType.DMA((4, 2)),
            ],
        ),
        out_shape=jax.ShapeDtypeStruct((4, 4, GROUP, 128), F32),
        name="sink_source",
    )(owner, field)


def contract_block(rows, b, slots, s_buf, h_buf, g_buf, sig, s_sum, h_sum, macc, mout):
    for u in range(78):
        part = []
        for e in (u, 78 + u):
            v = g_buf[b, slots[e // 39], e % 39 * rows : e % 39 * rows + rows, :]
            sig[(e // 78) * 78 + u, 0:rows, :] = v
            part.append(v)
        sig[156 + u, 0:rows, :] = part[0] + part[1]
    for e in range(144):
        s_sum[e] = s_buf[b, e] + s_buf[b, 144 + e]
        h_sum[e] = h_buf[b, e] + h_buf[b, 144 + e]

    def spin(alpha, carry):
        base = alpha * 36
        for nt in range(0, 12, 3):
            acc = {}
            for m in range(12):
                h = [
                    (h_buf[b, base + a * 12 + m], h_buf[b, base + (144 + a * 12 + m)], h_sum[base + a * 12 + m])
                    for a in range(3)
                ]
                for n in range(nt, nt + 3):
                    u = pair_index(m, n)
                    g = (sig[u], sig[78 + u], sig[156 + u])
                    for a in range(3):
                        new = tuple(x * y for x, y in zip(h[a], g))
                        acc[a, n] = new if m == 0 else tuple(x + y for x, y in zip(acc[a, n], new))
            conj = {}
            for key, (p1, p2, p3) in acc.items():
                u_, w_ = p1 - p2, p1 + p2 - p3
                conj[key] = (u_, w_, u_ + w_)
            for beta in range(4):
                q = None
                for (a, n), t in conj.items():
                    e = (3 * beta + a) * 12 + n
                    s = (s_buf[b, e], s_buf[b, 144 + e], s_sum[e])
                    new = tuple(x * y for x, y in zip(s, t))
                    q = new if q is None else tuple(x + y for x, y in zip(q, new))
                if nt > 0:
                    q = tuple(q[i] + macc[beta, i] for i in range(3))
                if nt < 9:
                    for i in range(3):
                        macc[beta, i] = q[i]
                else:
                    mout[alpha * 4 + beta] = q[0] - q[1]
                    mout[16 + alpha * 4 + beta] = q[2] - q[0] - q[1]
        return carry

    lax.fori_loop(0, 4, spin, 0)


def contract_kernel(rows, starts, nb, take, *refs):
    scal, prop, back, phases = refs[:4]
    sources = refs[4:-10]
    out_ref, s_buf, h_buf, g_buf, sig, s_sum, h_sum, macc, mout, sems = refs[-10:]

    def first_row(b):
        q = scal[b, 0]
        start = jnp.int32(starts[3])
        for i in range(3):
            start = jnp.where(q == i, starts[i], start)
        return start

    def copies(b):
        start = first_row(b)
        return [
            pltpu.make_async_copy(take(sources, b), g_buf.at[b], sems.at[b, 0]),
            block_copy(back, start, rows, h_buf.at[b], sems.at[b, 1]),
            block_copy(prop, start, rows, s_buf.at[b], sems.at[b, 2]),
        ]

    for b in range(nb):
        for copy in copies(b):
            copy.start()
    out_ref[...] = jnp.zeros_like(out_ref)

    def block(b, carry):
        for i in range(nb):

            @pl.when(b == i)
            def _():
                for copy in copies(i):
                    copy.wait()

        slots = [scal[b, 1 + g] for g in range(4)]
        contract_block(rows, b, slots, s_buf, h_buf, g_buf, sig, s_sum, h_sum, macc, mout)
        q = scal[b, 0]
        total = out_ref[...]
        for pair in range(rows // 2):
            wide = jnp.concatenate([mout[:, 2 * pair, :], mout[:, 2 * pair + 1, :]], axis=1)
            high = wide.astype(BF16)
            low = (wide - high.astype(F32)).astype(BF16)
            total += lax.dot_general(
                jnp.concatenate([high, low], axis=0),
                phases[q, pair],
                (((1,), (1,)), ((), ())),
                preferred_element_type=F32,
            )
        out_ref[...] = total
        return carry

    lax.fori_loop(0, nb, block, 0)


def contract(rows, nb, take, scal, prop, back, phases, sources, name):
    starts = A_START if rows == 8 else B_START

    def kernel(*refs):
        contract_kernel(rows, starts, nb, take, *refs)

    anywhere = pl.BlockSpec(memory_space=pl.ANY)
    return pl.pallas_call(
        kernel,
        in_specs=[pl.BlockSpec(memory_space=pltpu.SMEM), anywhere, anywhere, pl.BlockSpec(memory_space=pltpu.VMEM)]
        + [anywhere] * len(sources),
        out_specs=pl.BlockSpec(memory_space=pltpu.VMEM),
        out_shape=jax.ShapeDtypeStruct((64, 112), F32),
        scratch_shapes=[
            pltpu.VMEM((nb, 288, 8, 128), F32),
            pltpu.VMEM((nb, 288, 8, 128), F32),
            pltpu.VMEM((nb, 4, 40 * rows, 128), F32),
            pltpu.VMEM((234, 8, 128), F32),
            pltpu.VMEM((144, 8, 128), F32),
            pltpu.VMEM((144, 8, 128), F32),
            pltpu.VMEM((4, 3, 8, 128), F32),
            pltpu.VMEM((32, 8, 128), F32),
            pltpu.SemaphoreType.DMA((nb, 3)),
        ],
        name=name,
    )(scal, prop, back, phases, *sources)


def phase_blocks(rows, starts, first_site, source_position, momenta):
    shape = (4, rows // 2, 112, 256)
    row0 = np.array(starts, np.int32)[:, None, None, None]
    row = row0 + 2 * np.arange(rows // 2, dtype=np.int32)[None, :, None, None]
    lane = np.arange(256, dtype=np.int32)[None, None, None, :]
    row = row + lane // 128
    used = np.broadcast_to((row < ROWS) & ((row0 + np.zeros_like(row)) * 0 == 0), shape[:2] + (1, 256)).copy()
    if rows == 6:
        used[3, 0] = False
    site = jnp.asarray(row * 128 + lane % 128) + first_site
    column = np.arange(112) % 56
    vectors = jnp.concatenate([momenta, jnp.zeros((1, 3), jnp.int32)], axis=0)
    vectors = jnp.concatenate([vectors] * 4, axis=0)[None, None, :, :, None]
    wave = (
        vectors[:, :, :, 0] * (site // L % L - source_position[0])
        + vectors[:, :, :, 1] * (site % L - source_position[1])
        + vectors[:, :, :, 2] * (site // (L * L) - source_position[2])
    )
    turn = jnp.asarray(np.where(column < 28, 0, L // 4).astype(np.int32))[None, None, :, None]
    angle = jnp.mod(wave + turn, L).astype(F32) * (2.0 * math.pi / L)
    value = jnp.where(jnp.asarray(used), jnp.cos(angle), 0.0)
    high = lax.reduce_precision(value, 8, 7)
    is_high = jnp.asarray(np.arange(112) < 56)[None, None, :, None]
    return jnp.where(is_high, high, value - high).astype(BF16)


def finish_kernel(nparts, *refs):
    weights, out_ref = refs[0], refs[-1]
    total = refs[1][...]
    for part in refs[2 : 1 + nparts]:
        total += part[...]
    total = total[:32] + total[32:]
    total = total[:, :56] + total[:, 56:]
    cosine, sine = total[:, :28], total[:, 28:56]
    re = cosine[:16] - sine[16:]
    im = sine[:16] + cosine[16:]
    out_ref[...] = jnp.dot(
        weights[...],
        jnp.concatenate([re, im], axis=0),
        precision=lax.Precision.HIGHEST,
        preferred_element_type=F32,
    )


def finish(weights, parts):
    def kernel(*refs):
        finish_kernel(len(parts), *refs)

    return pl.pallas_call(
        kernel, out_shape=jax.ShapeDtypeStruct((32, 28), F32), name="currents"
    )(weights, *parts)


def body(propagator, backward, sink_time, source_position, momenta, gamma_table):
    prop = propagator.reshape(288, ROWS, 1, 128)
    back = backward.reshape(288, ROWS, 1, 128)
    core = lax.axis_index("gz")
    owner = (lax.axis_index("ta") == sink_time[0]).astype(jnp.int32)
    packed = source(owner[None], prop)

    first_site = core * (ROWS * 128)
    phases_a = phase_blocks(8, A_START, first_site, source_position, momenta)
    phases_b = phase_blocks(6, B_START, first_site, source_position, momenta)

    order = jnp.roll(gamma_table, -8 * core)
    chosen = (order[:, None] == jnp.arange(NG, dtype=jnp.int32)[None, :]).astype(F32)
    weights = jnp.einsum(
        "cg,xgk->cxk", chosen, jnp.asarray(gamma_weights()), precision=lax.Precision.HIGHEST
    ).reshape(32, 32)

    parts = []
    for chunk in range(2):
        field = lax.psum(packed[2 * chunk : 2 * chunk + 2], "ta")
        scal = jnp.asarray(np.array([[2 * chunk + i, 0, 1, 2, 3, 0, 0, 0] for i in range(2)], np.int32))
        for rows, phases in ((8, phases_a), (6, phases_b)):
            lo, hi = (0, 320) if rows == 8 else (320, 560)
            parts.append(
                contract(
                    rows,
                    2,
                    lambda s, b, lo=lo, hi=hi: s[0].at[b, :, lo:hi, :],
                    scal,
                    prop,
                    back,
                    phases,
                    [field],
                    f"contract_{chunk}_{rows}",
                )
            )
    sums = finish(weights, parts).reshape(2, 8, 2, 28)
    other = lax.ppermute(sums[1], "gz", [(0, 1), (1, 0)])
    result = (sums[0] + other)[:, :, :NP]
    return jnp.transpose(result, (1, 0, 2))[:, None]


def solution(mesh):
    in_specs = (
        P(None, None, None, "ta", "gz"),
        P(None, None, None, "ta", "gz"),
        P(),
        P(),
        P(),
        P(),
    )
    out_specs = P(None, "ta", "gz", None)
    return jax.shard_map(body, mesh=mesh, in_specs=in_specs, out_specs=out_specs, check_vma=False)
```

```python
import math

import jax
import jax.numpy as jnp
import numpy as np
from jax import lax
from jax.experimental import pallas as pl
from jax.experimental.pallas import tpu as pltpu
from jax.sharding import PartitionSpec as P

L = 24
NG = 16
NP = 27
ROWS = 54
A_START = (0, 14, 28, 42)
B_START = (8, 22, 36, 48)
GROUP = 560
F32 = jnp.float32
BF16 = jnp.bfloat16


def pair_index(m, n):
    m, n = min(m, n), max(m, n)
    return m * 12 - m * (m - 1) // 2 + (n - m)


def gamma_weights():
    paulis = [
        np.eye(2),
        np.array([[0.0, 1.0], [1.0, 0.0]]),
        np.array([[0.0, -1j], [1j, 0.0]]),
        np.array([[1.0, 0.0], [0.0, -1.0]]),
    ]
    matrices = np.stack([np.kron(paulis[number // 4], paulis[number % 4]) for number in range(16)])
    flat = matrices.reshape(16, 16) / (72.0 * math.sqrt(L * L * L))
    top = np.concatenate([flat.real, -flat.imag], axis=1)
    low = np.concatenate([flat.imag, flat.real], axis=1)
    return np.stack([top, low]).astype(np.float32)


def block_copy(field, start, rows, buf, sem):
    return pltpu.make_async_copy(
        field.at[:, pl.ds(start, rows), 0, :], buf.at[:, pl.ds(0, rows), :], sem
    )


def source_block(buf, sums, write):
    for e in range(144):
        sums[e] = buf[e] + buf[144 + e]
    for mt in range(0, 12, 3):
        for nt in range(mt, 12, 3):
            pairs = [(m, n) for m in range(mt, mt + 3) for n in range(nt, nt + 3) if m <= n]
            acc = {}
            for k in range(12):
                rows = sorted({m for m, _ in pairs} | {n for _, n in pairs})
                re = {m: buf[m * 12 + k] for m in rows}
                im = {m: buf[144 + m * 12 + k] for m in rows}
                su = {m: sums[m * 12 + k] for m in rows}
                for m, n in pairs:
                    new = (re[m] * re[n], im[m] * im[n], su[m] * su[n])
                    acc[m, n] = new if k == 0 else tuple(a + b for a, b in zip(acc[m, n], new))
            for m, n in pairs:
                p1, p2, p3 = acc[m, n]
                write(pair_index(m, n), 0.125 * (p1 - p2), 0.125 * (p3 - p1 - p2))


def source_kernel(q, owner_ref, field, out_ref, buf_a, buf_b, sums, sems):
    @pl.when(owner_ref[0] == 1)
    def _():
        copy_a = block_copy(field, A_START[q], 8, buf_a, sems.at[0])
        copy_b = block_copy(field, B_START[q], 6, buf_b, sems.at[1])
        copy_a.start()
        copy_b.start()

        def write_a(u, re, im):
            for e, v in ((u, re), (78 + u, im)):
                out_ref[e // 39, e % 39 * 8 : e % 39 * 8 + 8, :] = v

        def write_b(u, re, im):
            for e, v in ((u, re), (78 + u, im)):
                out_ref[e // 39, 320 + e % 39 * 6 : 320 + e % 39 * 6 + 6, :] = v[:6]

        copy_a.wait()
        source_block(buf_a, sums, write_a)
        copy_b.wait()
        source_block(buf_b, sums, write_b)


def source(q, owner, field):
    def kernel(*refs):
        source_kernel(q, *refs)

    return pl.pallas_call(
        kernel,
        in_specs=[pl.BlockSpec(memory_space=pltpu.SMEM), pl.BlockSpec(memory_space=pl.ANY)],
        out_specs=pl.BlockSpec(memory_space=pltpu.VMEM),
        out_shape=jax.ShapeDtypeStruct((4, GROUP, 128), F32),
        scratch_shapes=[
            pltpu.VMEM((288, 8, 128), F32),
            pltpu.VMEM((288, 8, 128), F32),
            pltpu.VMEM((144, 8, 128), F32),
            pltpu.SemaphoreType.DMA((2,)),
        ],
        name=f"sink_source_{q}",
    )(owner, field)


STRIDE = {"y": 16, "x": 4, "z": 1}
AXES = ((("x", 1), ("y", 1), ("z", 1)), (("y", -1), ("z", -1), ("x", -1)))
UNIT = ((1, 0, 0), (0, 1, 0), (0, 0, 1))
TWICE = ((2, 0, 0), (0, 2, 0), (0, 0, 2))
DIAGONAL = ((1, 1, 1), (2, 2, 2), (3, 3, 3))


def moved(vector):
    pairs = []
    for place in range(64):
        for core in range(2):
            target = place
            for (axis, sign), step in zip(AXES[core], vector):
                digit = place // STRIDE[axis] % 4
                target += ((digit + sign * step) % 4 - digit) * STRIDE[axis]
            pairs.append((2 * place + core, 2 * target + core))
    return pairs


def shift(value, vector):
    return lax.ppermute(value, ("ta", "gz"), moved(vector))


def relative(sink_time):
    here, there = lax.axis_index("ta"), sink_time[0]
    core = lax.axis_index("gz")
    digits = {"y": 4, "x": 2, "z": 0}
    steps = {a: (here >> n) - (there >> n) for a, n in digits.items()}
    out = []
    for i in range(3):
        (a0, s0), (a1, s1) = AXES[0][i], AXES[1][i]
        out.append(jnp.where(core == 0, s0 * steps[a0], s1 * steps[a1]) & 3)
    return out


def labels_at(u, v, w):
    c = ((u + w) & 1) + 2 * ((v + w) & 1)
    hu = (u - (c == 1)) & 3
    hv = (v - (c == 2)) & 3
    hw = (w - (c == 3)) & 3
    d = ((hu >> 1) ^ (hw >> 1)) + 2 * ((hv >> 1) ^ (hw >> 1))
    copy = (hu - 2 * (d == 1)) & 3
    return c, d, copy


def pick(index, sources):
    value = sources[-1]
    for i in range(len(sources) - 2, -1, -1):
        value = jnp.where(index == i, sources[i], value)
    return value


def spread(quarters, sink_time):
    u, v, w = relative(sink_time)
    c, d, copy = labels_at(u, v, w)
    got = {k: shift(quarters[k], UNIT[k - 1]) for k in (1, 2, 3)}
    arrived = [quarters[0]] + [got[k] for k in (1, 2, 3)]
    groups = [pick(c, [a[g] for a in arrived]) for g in range(4)]
    got = [shift(groups[k], TWICE[k - 1]) for k in (1, 2, 3)]
    piece = pick(d, [groups[0]] + got)
    got = [shift(piece, DIAGONAL[k - 1]) for k in (1, 2, 3)]
    piece = pick(copy, [piece] + got)
    groups = [piece] + [shift(piece, TWICE[k - 1]) for k in (1, 2, 3)]
    upper = jnp.concatenate([g[:320] for g in groups]).reshape(4, 320, 128)
    lower = jnp.concatenate([g[320:] for g in groups]).reshape(4, 240, 128)
    upper_got = [shift(upper, UNIT[k]) for k in range(3)]
    lower_got = [shift(lower, UNIT[k]) for k in range(3)]
    rows = []
    for step in ((0, 0, 0),) + UNIT:
        c, d, _ = labels_at((u - step[0]) & 3, (v - step[1]) & 3, (w - step[2]) & 3)
        rows.append(jnp.stack([c, d, d ^ 1, d ^ 2, d ^ 3]))
    return [upper] + upper_got, [lower] + lower_got, jnp.stack(rows).astype(jnp.int32)


def contract_block(rows, b, slots, s_buf, h_buf, g_buf, sig, s_sum, h_sum, macc, mout):
    for u in range(78):
        part = []
        for e in (u, 78 + u):
            v = g_buf[b, slots[e // 39], e % 39 * rows : e % 39 * rows + rows, :]
            sig[(e // 78) * 78 + u, 0:rows, :] = v
            part.append(v)
        sig[156 + u, 0:rows, :] = part[0] + part[1]
    for e in range(144):
        s_sum[e] = s_buf[b, e] + s_buf[b, 144 + e]
        h_sum[e] = h_buf[b, e] + h_buf[b, 144 + e]

    def spin(alpha, carry):
        base = alpha * 36
        for nt in range(0, 12, 3):
            acc = {}
            for m in range(12):
                h = [
                    (h_buf[b, base + a * 12 + m], h_buf[b, base + (144 + a * 12 + m)], h_sum[base + a * 12 + m])
                    for a in range(3)
                ]
                for n in range(nt, nt + 3):
                    u = pair_index(m, n)
                    g = (sig[u], sig[78 + u], sig[156 + u])
                    for a in range(3):
                        new = tuple(x * y for x, y in zip(h[a], g))
                        acc[a, n] = new if m == 0 else tuple(x + y for x, y in zip(acc[a, n], new))
            conj = {}
            for key, (p1, p2, p3) in acc.items():
                u_, w_ = p1 - p2, p1 + p2 - p3
                conj[key] = (u_, w_, u_ + w_)
            for beta in range(4):
                q = None
                for (a, n), t in conj.items():
                    e = (3 * beta + a) * 12 + n
                    s = (s_buf[b, e], s_buf[b, 144 + e], s_sum[e])
                    new = tuple(x * y for x, y in zip(s, t))
                    q = new if q is None else tuple(x + y for x, y in zip(q, new))
                if nt > 0:
                    q = tuple(q[i] + macc[beta, i] for i in range(3))
                if nt < 9:
                    for i in range(3):
                        macc[beta, i] = q[i]
                else:
                    mout[alpha * 4 + beta] = q[0] - q[1]
                    mout[16 + alpha * 4 + beta] = q[2] - q[0] - q[1]
        return carry

    lax.fori_loop(0, 4, spin, 0)


def contract_kernel(rows, starts, nb, take, *refs):
    scal, prop, back, phases = refs[:4]
    sources = refs[4:-10]
    out_ref, s_buf, h_buf, g_buf, sig, s_sum, h_sum, macc, mout, sems = refs[-10:]

    def first_row(b):
        q = scal[b, 0]
        start = jnp.int32(starts[3])
        for i in range(3):
            start = jnp.where(q == i, starts[i], start)
        return start

    def copies(b):
        start = first_row(b)
        return [
            pltpu.make_async_copy(take(sources, b), g_buf.at[b], sems.at[b, 0]),
            block_copy(back, start, rows, h_buf.at[b], sems.at[b, 1]),
            block_copy(prop, start, rows, s_buf.at[b], sems.at[b, 2]),
        ]

    for b in range(nb):
        for copy in copies(b):
            copy.start()
    out_ref[...] = jnp.zeros_like(out_ref)

    def block(b, carry):
        for i in range(nb):

            @pl.when(b == i)
            def _():
                for copy in copies(i):
                    copy.wait()

        slots = [scal[b, 1 + g] for g in range(4)]
        contract_block(rows, b, slots, s_buf, h_buf, g_buf, sig, s_sum, h_sum, macc, mout)
        q = scal[b, 0]
        total = out_ref[...]
        for pair in range(rows // 2):
            wide = jnp.concatenate([mout[:, 2 * pair, :], mout[:, 2 * pair + 1, :]], axis=1)
            high = wide.astype(BF16)
            low = (wide - high.astype(F32)).astype(BF16)
            total += lax.dot_general(
                jnp.concatenate([high, low], axis=0),
                phases[q, pair],
                (((1,), (1,)), ((), ())),
                preferred_element_type=F32,
            )
        out_ref[...] = total
        return carry

    lax.fori_loop(0, nb, block, 0)


def contract(rows, nb, take, scal, prop, back, phases, sources, name):
    starts = A_START if rows == 8 else B_START

    def kernel(*refs):
        contract_kernel(rows, starts, nb, take, *refs)

    anywhere = pl.BlockSpec(memory_space=pl.ANY)
    return pl.pallas_call(
        kernel,
        in_specs=[pl.BlockSpec(memory_space=pltpu.SMEM), anywhere, anywhere, pl.BlockSpec(memory_space=pltpu.VMEM)]
        + [anywhere] * len(sources),
        out_specs=pl.BlockSpec(memory_space=pltpu.VMEM),
        out_shape=jax.ShapeDtypeStruct((64, 112), F32),
        scratch_shapes=[
            pltpu.VMEM((nb, 288, 8, 128), F32),
            pltpu.VMEM((nb, 288, 8, 128), F32),
            pltpu.VMEM((nb, 4, 40 * rows, 128), F32),
            pltpu.VMEM((234, 8, 128), F32),
            pltpu.VMEM((144, 8, 128), F32),
            pltpu.VMEM((144, 8, 128), F32),
            pltpu.VMEM((4, 3, 8, 128), F32),
            pltpu.VMEM((32, 8, 128), F32),
            pltpu.SemaphoreType.DMA((nb, 3)),
        ],
        name=name,
    )(scal, prop, back, phases, *sources)


def quarter_turns(wave):
    wave = wave - 24.0 * jnp.floor((wave + 0.5) * (1.0 / 24.0))
    t = (jnp.abs(wave - 12.0) - 6.0) * (math.pi / 12.0)
    t2 = t * t
    value = t2 * (1.0 / 6227020800.0) - 1.0 / 39916800.0
    for k in (362880.0, -5040.0, 120.0, -6.0):
        value = value * t2 + 1.0 / k
    return t + t * (t2 * value)


def phase_blocks(rows, starts, core, source_position, momenta):
    row = np.array(starts, np.int32)[:, None, None, None]
    row = row + 2 * np.arange(rows // 2, dtype=np.int32)[None, :, None, None]
    lane = np.arange(256, dtype=np.int32)[None, None, None, :]
    row = row + lane // 128
    used = np.ones(row.shape, np.float32)
    if rows == 6:
        used[3, 0] = 0.0
    site = row * 128 + lane % 128
    place = source_position.astype(F32)
    xs = jnp.asarray((site // L % L).astype(np.float32)) - place[0]
    ys = jnp.asarray((site % L).astype(np.float32)) - place[1]
    zs = jnp.asarray((site // (L * L)).astype(np.float32)) + (12.0 * core.astype(F32) - place[2])
    vectors = jnp.concatenate([momenta, jnp.zeros((1, 3), jnp.int32)], axis=0).astype(F32)
    vectors = jnp.concatenate([vectors] * 4, axis=0)[None, None, :, :, None]
    turn = np.where(np.arange(112) % 56 < 28, 0.0, 6.0).astype(np.float32)
    wave = (
        vectors[:, :, :, 0] * xs
        + vectors[:, :, :, 1] * ys
        + vectors[:, :, :, 2] * zs
        + jnp.asarray(turn)[None, None, :, None]
    )
    value = quarter_turns(wave) * jnp.asarray(used)
    high = lax.reduce_precision(value, 8, 7)
    is_high = jnp.asarray(np.arange(112) < 56)[None, None, :, None]
    return jnp.where(is_high, high, value - high).astype(BF16)


def finish_kernel(nparts, *refs):
    weights, out_ref = refs[0], refs[-1]
    total = refs[1][...]
    for part in refs[2 : 1 + nparts]:
        total += part[...]
    total = total[:32] + total[32:]
    total = total[:, :56] + total[:, 56:]
    cosine, sine = total[:, :28], total[:, 28:56]
    re = cosine[:16] - sine[16:]
    im = sine[:16] + cosine[16:]
    out_ref[...] = jnp.dot(
        weights[...],
        jnp.concatenate([re, im], axis=0),
        precision=lax.Precision.HIGHEST,
        preferred_element_type=F32,
    )


def finish(weights, parts):
    def kernel(*refs):
        finish_kernel(len(parts), *refs)

    return pl.pallas_call(
        kernel, out_shape=jax.ShapeDtypeStruct((32, 28), F32), name="currents"
    )(weights, *parts)


def body(propagator, backward, sink_time, source_position, momenta, gamma_table):
    prop = propagator.reshape(288, ROWS, 1, 128)
    back = backward.reshape(288, ROWS, 1, 128)
    core = lax.axis_index("gz")
    owner = (lax.axis_index("ta") == sink_time[0]).astype(jnp.int32)
    quarters = {q: source(q, owner[None], prop) for q in (1, 2, 3, 0)}

    phases_a = phase_blocks(8, A_START, core, source_position, momenta)
    phases_b = phase_blocks(6, B_START, core, source_position, momenta)

    order = jnp.roll(gamma_table, -8 * core)
    chosen = (order[:, None] == jnp.arange(NG, dtype=jnp.int32)[None, :]).astype(F32)
    weights = jnp.einsum(
        "cg,xgk->cxk", chosen, jnp.asarray(gamma_weights()), precision=lax.Precision.HIGHEST
    ).reshape(32, 32)

    upper, lower, labels = spread(quarters, sink_time)
    parts = []
    for first, last in ((0, 1), (1, 4)):
        for rows, phases, fields in ((8, phases_a, upper), (6, phases_b, lower)):
            parts.append(
                contract(
                    rows,
                    last - first,
                    lambda s, b: s[b],
                    labels[first:last],
                    prop,
                    back,
                    phases,
                    fields[first:last],
                    f"contract_{first}_{rows}",
                )
            )
    sums = finish(weights, parts).reshape(2, 8, 2, 28)
    other = lax.ppermute(sums[1], "gz", [(0, 1), (1, 0)])
    result = (sums[0] + other)[:, :, :NP]
    return jnp.transpose(result, (1, 0, 2))[:, None]


def solution(mesh):
    in_specs = (
        P(None, None, None, "ta", "gz"),
        P(None, None, None, "ta", "gz"),
        P(),
        P(),
        P(),
        P(),
    )
    out_specs = P(None, "ta", "gz", None)
    return jax.shard_map(body, mesh=mesh, in_specs=in_specs, out_specs=out_specs, check_vma=False)
```

```python
import math

import jax
import jax.numpy as jnp
import numpy as np
from jax import lax
from jax.experimental import pallas as pl
from jax.experimental.pallas import tpu as pltpu
from jax.sharding import PartitionSpec as P

L = 24
NG = 16
NP = 27
ROWS = 54
A_START = (0, 14, 28, 42)
B_START = (8, 22, 36, 48)
GROUP = 560
F32 = jnp.float32
BF16 = jnp.bfloat16


def pair_index(m, n):
    m, n = min(m, n), max(m, n)
    return m * 12 - m * (m - 1) // 2 + (n - m)


def gamma_weights():
    paulis = [
        np.eye(2),
        np.array([[0.0, 1.0], [1.0, 0.0]]),
        np.array([[0.0, -1j], [1j, 0.0]]),
        np.array([[1.0, 0.0], [0.0, -1.0]]),
    ]
    matrices = np.stack([np.kron(paulis[number // 4], paulis[number % 4]) for number in range(16)])
    flat = matrices.reshape(16, 16) / (72.0 * math.sqrt(L * L * L))
    top = np.concatenate([flat.real, -flat.imag], axis=1)
    low = np.concatenate([flat.imag, flat.real], axis=1)
    return np.stack([top, low]).astype(np.float32)


def block_copy(field, start, rows, buf, sem):
    return pltpu.make_async_copy(
        field.at[:, pl.ds(start, rows), 0, :], buf.at[:, pl.ds(0, rows), :], sem
    )


def source_block(buf, sums, write):
    for e in range(144):
        sums[e] = buf[e] + buf[144 + e]
    for mt in range(0, 12, 3):
        for nt in range(mt, 12, 3):
            pairs = [(m, n) for m in range(mt, mt + 3) for n in range(nt, nt + 3) if m <= n]
            acc = {}
            for k in range(12):
                rows = sorted({m for m, _ in pairs} | {n for _, n in pairs})
                re = {m: buf[m * 12 + k] for m in rows}
                im = {m: buf[144 + m * 12 + k] for m in rows}
                su = {m: sums[m * 12 + k] for m in rows}
                for m, n in pairs:
                    new = (re[m] * re[n], im[m] * im[n], su[m] * su[n])
                    acc[m, n] = new if k == 0 else tuple(a + b for a, b in zip(acc[m, n], new))
            for m, n in pairs:
                p1, p2, p3 = acc[m, n]
                write(pair_index(m, n), 0.125 * (p1 - p2), 0.125 * (p3 - p1 - p2))


def source_kernel(quarters, owner_ref, field, *refs):
    outs = refs[: len(quarters)]
    bufs, stage, sums, sems, out_sems = refs[len(quarters) :]

    @pl.when(owner_ref[0] == 1)
    def _():
        blocks = [(i, half) for i in range(len(quarters)) for half in range(2)]

        def copy_in(number):
            i, half = blocks[number]
            start = (A_START, B_START)[half][quarters[i]]
            return block_copy(field, start, 8 - 2 * half, bufs.at[number], sems.at[number])

        def copy_out(i):
            return pltpu.make_async_copy(stage.at[i], outs[i], out_sems.at[i])

        copy_in(0).start()
        copy_in(1).start()
        for number, (i, half) in enumerate(blocks):
            copy_in(number).wait()
            if number + 2 < len(blocks):
                copy_in(number + 2).start()

            def write(u, re, im, i=i, half=half):
                rows = 8 - 2 * half
                for e, v in ((u, re), (78 + u, im)):
                    first = 320 * half + e % 39 * rows
                    stage[i, e // 39, first : first + rows, :] = v[:rows]

            source_block(bufs.at[number], sums, write)
            if half == 1:
                copy_out(i).start()
        for i in range(len(quarters)):
            copy_out(i).wait()


def source(quarters, owner, field):
    count = len(quarters)

    def kernel(*refs):
        source_kernel(quarters, *refs)

    anywhere = pl.BlockSpec(memory_space=pl.ANY)
    return pl.pallas_call(
        kernel,
        in_specs=[pl.BlockSpec(memory_space=pltpu.SMEM), anywhere],
        out_specs=[anywhere] * count,
        out_shape=[jax.ShapeDtypeStruct((4, GROUP, 128), F32)] * count,
        scratch_shapes=[
            pltpu.VMEM((2 * count, 288, 8, 128), F32),
            pltpu.VMEM((count, 4, GROUP, 128), F32),
            pltpu.VMEM((144, 8, 128), F32),
            pltpu.SemaphoreType.DMA((2 * count,)),
            pltpu.SemaphoreType.DMA((count,)),
        ],
        name=f"sink_source_{quarters[0]}",
    )(owner, field)


STRIDE = {"y": 16, "x": 4, "z": 1}
AXES = ((("x", 1), ("y", 1), ("z", 1)), (("y", -1), ("z", -1), ("x", -1)))
UNIT = ((1, 0, 0), (0, 1, 0), (0, 0, 1))
TWICE = ((2, 0, 0), (0, 2, 0), (0, 0, 2))
DIAGONAL = ((1, 1, 1), (2, 2, 2), (3, 3, 3))


def moved(vector):
    pairs = []
    for place in range(64):
        for core in range(2):
            target = place
            for (axis, sign), step in zip(AXES[core], vector):
                digit = place // STRIDE[axis] % 4
                target += ((digit + sign * step) % 4 - digit) * STRIDE[axis]
            pairs.append((2 * place + core, 2 * target + core))
    return pairs


def shift(value, vector):
    return lax.ppermute(value, ("ta", "gz"), moved(vector))


def relative(sink_time):
    here, there = lax.axis_index("ta"), sink_time[0]
    core = lax.axis_index("gz")
    digits = {"y": 4, "x": 2, "z": 0}
    steps = {a: (here >> n) - (there >> n) for a, n in digits.items()}
    out = []
    for i in range(3):
        (a0, s0), (a1, s1) = AXES[0][i], AXES[1][i]
        out.append(jnp.where(core == 0, s0 * steps[a0], s1 * steps[a1]) & 3)
    return out


def labels_at(u, v, w):
    c = ((u + w) & 1) + 2 * ((v + w) & 1)
    hu = (u - (c == 1)) & 3
    hv = (v - (c == 2)) & 3
    hw = (w - (c == 3)) & 3
    d = ((hu >> 1) ^ (hw >> 1)) + 2 * ((hv >> 1) ^ (hw >> 1))
    copy = (hu - 2 * (d == 1)) & 3
    return c, d, copy


def pick(index, sources):
    value = sources[-1]
    for i in range(len(sources) - 2, -1, -1):
        value = jnp.where(index == i, sources[i], value)
    return value


def spread(quarters, sink_time, ready):
    u, v, w = relative(sink_time)
    c, d, copy = labels_at(u, v, w)
    rows = []
    for step in ((0, 0, 0),) + UNIT:
        qc, qd, _ = labels_at((u - step[0]) & 3, (v - step[1]) & 3, (w - step[2]) & 3)
        rows.append(jnp.stack([qc, qd, qd ^ 1, qd ^ 2, qd ^ 3]))
    labels = jnp.stack(rows).astype(jnp.int32)
    arrived = [quarters[0]] + [shift(quarters[k], UNIT[k - 1]) for k in (1, 2, 3)]
    c, labels, ready = lax.optimization_barrier((c, labels, ready))
    groups = [pick(c, [a[g] for a in arrived]) for g in range(4)]
    got = [shift(groups[k], TWICE[k - 1]) for k in (1, 2, 3)]
    piece = pick(d, [groups[0]] + got)
    got = [shift(piece, DIAGONAL[k - 1]) for k in (1, 2, 3)]
    piece = pick(copy, [piece] + got)
    own = jnp.stack([piece] + [shift(piece, TWICE[k - 1]) for k in (1, 2, 3)])
    return [own] + [shift(own, UNIT[k]) for k in range(3)], labels, ready


def contract_block(rows, b, slots, s_buf, h_buf, g_buf, sig, s_sum, h_sum, macc, mout):
    for u in range(78):
        part = []
        for e in (u, 78 + u):
            v = g_buf[b, slots[e // 39], e % 39 * rows : e % 39 * rows + rows, :]
            sig[(e // 78) * 78 + u, 0:rows, :] = v
            part.append(v)
        sig[156 + u, 0:rows, :] = part[0] + part[1]
    for e in range(144):
        s_sum[e] = s_buf[b, e] + s_buf[b, 144 + e]
        h_sum[e] = h_buf[b, e] + h_buf[b, 144 + e]

    def spin(alpha, carry):
        base = alpha * 36
        for nt in range(0, 12, 3):
            acc = {}
            for m in range(12):
                h = [
                    (h_buf[b, base + a * 12 + m], h_buf[b, base + (144 + a * 12 + m)], h_sum[base + a * 12 + m])
                    for a in range(3)
                ]
                for n in range(nt, nt + 3):
                    u = pair_index(m, n)
                    g = (sig[u], sig[78 + u], sig[156 + u])
                    for a in range(3):
                        new = tuple(x * y for x, y in zip(h[a], g))
                        acc[a, n] = new if m == 0 else tuple(x + y for x, y in zip(acc[a, n], new))
            conj = {}
            for key, (p1, p2, p3) in acc.items():
                u_, w_ = p1 - p2, p1 + p2 - p3
                conj[key] = (u_, w_, u_ + w_)
            for beta in range(4):
                q = None
                for (a, n), t in conj.items():
                    e = (3 * beta + a) * 12 + n
                    s = (s_buf[b, e], s_buf[b, 144 + e], s_sum[e])
                    new = tuple(x * y for x, y in zip(s, t))
                    q = new if q is None else tuple(x + y for x, y in zip(q, new))
                if nt > 0:
                    q = tuple(q[i] + macc[beta, i] for i in range(3))
                if nt < 9:
                    for i in range(3):
                        macc[beta, i] = q[i]
                else:
                    mout[alpha * 4 + beta] = q[0] - q[1]
                    mout[16 + alpha * 4 + beta] = q[2] - q[0] - q[1]
        return carry

    lax.fori_loop(0, 4, spin, 0)


def project(rows, mout, phases, total):
    for pair in range(rows // 2):
        wide = jnp.concatenate([mout[:, 2 * pair, :], mout[:, 2 * pair + 1, :]], axis=1)
        high = wide.astype(BF16)
        low = (wide - high.astype(F32)).astype(BF16)
        total += lax.dot_general(
            jnp.concatenate([high, low], axis=0),
            phases[pair],
            (((1,), (1,)), ((), ())),
            preferred_element_type=F32,
        )
    return total


def currents(weights, total):
    total = total[:32] + total[32:]
    total = total[:, :56] + total[:, 56:]
    cosine, sine = total[:, :28], total[:, 28:56]
    re = cosine[:16] - sine[16:]
    im = sine[:16] + cosine[16:]
    return jnp.dot(
        weights,
        jnp.concatenate([re, im], axis=0),
        precision=lax.Precision.HIGHEST,
        preferred_element_type=F32,
    )


def contract_kernel(nf, last, scal, prop, back, phases_a, phases_b, *refs):
    fields, refs = refs[:nf], refs[nf:]
    if last:
        before, weights, keep_ref, send_ref = refs[:4]
        refs = refs[4:]
    else:
        out_ref, refs = refs[0], refs[1:]
    s_buf, h_buf, g_buf, p_buf, sig, s_sum, h_sum, macc, mout, acc, sems = refs
    nb = 2 * nf

    def first_row(starts, b):
        q = scal[b % nf, 0]
        start = jnp.int32(starts[3])
        for i in range(3):
            start = jnp.where(q == i, starts[i], start)
        return start

    def copies(b):
        half = b // nf
        rows, lo = (8, 0) if half == 0 else (6, 320)
        starts, phases = ((A_START, phases_a), (B_START, phases_b))[half]
        start = first_row(starts, b)
        return [
            pltpu.make_async_copy(
                fields[b % nf].at[:, pl.ds(lo, 40 * rows), :],
                g_buf.at[b, :, pl.ds(0, 40 * rows), :],
                sems.at[b, 0],
            ),
            block_copy(back, start, rows, h_buf.at[b], sems.at[b, 1]),
            block_copy(prop, start, rows, s_buf.at[b], sems.at[b, 2]),
            pltpu.make_async_copy(
                phases.at[scal[b % nf, 0]], p_buf.at[b, pl.ds(0, rows // 2)], sems.at[b, 3]
            ),
        ]

    def on(b, action):
        for i in range(nb):

            @pl.when(b == i)
            def _():
                for copy in copies(i):
                    action(copy)

    for copy in copies(0):
        copy.start()
    acc[...] = before[...] if last else jnp.zeros_like(acc)
    for half, rows in ((0, 8), (1, 6)):

        def block(i, carry, half=half, rows=rows):
            b = half * nf + i
            on(b, lambda copy: copy.wait())
            on(b + 1, lambda copy: copy.start())
            slots = [scal[i, 1 + g] for g in range(4)]
            contract_block(rows, b, slots, s_buf, h_buf, g_buf, sig, s_sum, h_sum, macc, mout)
            acc[...] = project(rows, mout, p_buf.at[b], acc[...])
            return carry

        lax.fori_loop(0, nf, block, 0)
    if last:
        result = currents(weights[...], acc[...])
        keep_ref[...] = result[:16]
        send_ref[...] = result[16:]
    else:
        out_ref[...] = acc[...]


def contract(labels, prop, back, phases_a, phases_b, fields, before=None, weights=None):
    nf = len(fields)
    last = weights is not None

    def kernel(*refs):
        contract_kernel(nf, last, *refs)

    anywhere = pl.BlockSpec(memory_space=pl.ANY)
    vmem = pl.BlockSpec(memory_space=pltpu.VMEM)
    if last:
        out_shape = [jax.ShapeDtypeStruct((16, 28), F32)] * 2
    else:
        out_shape = [jax.ShapeDtypeStruct((64, 112), F32)]
    return pl.pallas_call(
        kernel,
        in_specs=[pl.BlockSpec(memory_space=pltpu.SMEM)] + [anywhere] * (4 + nf) + [vmem] * (2 * last),
        out_specs=[vmem] * len(out_shape),
        out_shape=out_shape,
        scratch_shapes=[
            pltpu.VMEM((2 * nf, 288, 8, 128), F32),
            pltpu.VMEM((2 * nf, 288, 8, 128), F32),
            pltpu.VMEM((2 * nf, 4, 320, 128), F32),
            pltpu.VMEM((2 * nf, 4, 112, 256), BF16),
            pltpu.VMEM((234, 8, 128), F32),
            pltpu.VMEM((144, 8, 128), F32),
            pltpu.VMEM((144, 8, 128), F32),
            pltpu.VMEM((4, 3, 8, 128), F32),
            pltpu.VMEM((32, 8, 128), F32),
            pltpu.VMEM((64, 112), F32),
            pltpu.SemaphoreType.DMA((2 * nf, 4)),
        ],
        name=f"contract_{nf}",
    )(labels, prop, back, phases_a, phases_b, *fields, *([before, weights] if last else []))


def quarter_turns(wave):
    wave = wave - 24.0 * jnp.floor((wave + 0.5) * (1.0 / 24.0))
    t = (jnp.abs(wave - 12.0) - 6.0) * (math.pi / 12.0)
    t2 = t * t
    value = t2 * (1.0 / 6227020800.0) - 1.0 / 39916800.0
    for k in (362880.0, -5040.0, 120.0, -6.0):
        value = value * t2 + 1.0 / k
    return t + t * (t2 * value)


def phase_blocks(rows, starts, core, source_position, momenta):
    row = np.array(starts, np.int32)[:, None, None, None]
    row = row + 2 * np.arange(rows // 2, dtype=np.int32)[None, :, None, None]
    lane = np.arange(256, dtype=np.int32)[None, None, None, :]
    row = row + lane // 128
    used = np.ones(row.shape, np.float32)
    if rows == 6:
        used[3, 0] = 0.0
    site = row * 128 + lane % 128
    place = source_position.astype(F32)
    xs = jnp.asarray((site // L % L).astype(np.float32)) - place[0]
    ys = jnp.asarray((site % L).astype(np.float32)) - place[1]
    zs = jnp.asarray((site // (L * L)).astype(np.float32)) + (12.0 * core.astype(F32) - place[2])
    vectors = jnp.concatenate([momenta, jnp.zeros((1, 3), jnp.int32)], axis=0).astype(F32)
    vectors = jnp.concatenate([vectors] * 4, axis=0)[None, None, :, :, None]
    turn = np.where(np.arange(112) % 56 < 28, 0.0, 6.0).astype(np.float32)
    wave = (
        vectors[:, :, :, 0] * xs
        + vectors[:, :, :, 1] * ys
        + vectors[:, :, :, 2] * zs
        + jnp.asarray(turn)[None, None, :, None]
    )
    value = quarter_turns(wave) * jnp.asarray(used)
    high = lax.reduce_precision(value, 8, 7)
    is_high = jnp.asarray(np.arange(112) < 56)[None, None, :, None]
    return jnp.where(is_high, high, value - high).astype(BF16)


def body(propagator, backward, sink_time, source_position, momenta, gamma_table):
    prop = propagator.reshape(288, ROWS, 1, 128)
    back = backward.reshape(288, ROWS, 1, 128)
    core = lax.axis_index("gz")
    owner = (lax.axis_index("ta") == sink_time[0]).astype(jnp.int32)
    quarters = dict(zip((1, 2, 3), source((1, 2, 3), owner[None], prop)))
    (quarters[0],) = source((0,), owner[None], prop)

    phases_a = phase_blocks(8, A_START, core, source_position, momenta)
    phases_b = phase_blocks(6, B_START, core, source_position, momenta)
    order = jnp.roll(gamma_table, -8 * core)
    chosen = (order[:, None] == jnp.arange(NG, dtype=jnp.int32)[None, :]).astype(F32)
    weights = jnp.einsum(
        "cg,xgk->cxk", chosen, jnp.asarray(gamma_weights()), precision=lax.Precision.HIGHEST
    ).reshape(32, 32)

    fields, labels, (phases_a, phases_b, weights) = spread(
        quarters, sink_time, (phases_a, phases_b, weights)
    )
    (own,) = contract(labels[:1], prop, back, phases_a, phases_b, fields[:1])
    keep, send = contract(labels[1:], prop, back, phases_a, phases_b, fields[1:], own, weights)
    result = keep + lax.ppermute(send, "gz", [(0, 1), (1, 0)])
    return jnp.transpose(result.reshape(8, 2, 28)[:, :, :NP], (1, 0, 2))[:, None]


def solution(mesh):
    in_specs = (
        P(None, None, None, "ta", "gz"),
        P(None, None, None, "ta", "gz"),
        P(),
        P(),
        P(),
        P(),
    )
    out_specs = P(None, "ta", "gz", None)
    return jax.shard_map(body, mesh=mesh, in_specs=in_specs, out_specs=out_specs, check_vma=False)
```

```python
import math

import jax
import jax.numpy as jnp
import numpy as np
from jax import lax
from jax.experimental import pallas as pl
from jax.experimental.pallas import tpu as pltpu
from jax.sharding import PartitionSpec as P

L = 24
NP = 27
ROWS = 54
A_START = (0, 14, 28, 42)
B_START = (8, 22, 36, 48)
GROUP = 560
F32 = jnp.float32
BF16 = jnp.bfloat16


def pair_index(m, n):
    m, n = min(m, n), max(m, n)
    return m * 12 - m * (m - 1) // 2 + (n - m)


def gamma_weights():
    paulis = [
        np.eye(2),
        np.array([[0.0, 1.0], [1.0, 0.0]]),
        np.array([[0.0, -1j], [1j, 0.0]]),
        np.array([[1.0, 0.0], [0.0, -1.0]]),
    ]
    matrices = np.stack([np.kron(paulis[number // 4], paulis[number % 4]) for number in range(16)])
    flat = matrices.reshape(16, 16) / (72.0 * math.sqrt(L * L * L))
    top = np.concatenate([flat.real, -flat.imag], axis=1)
    low = np.concatenate([flat.imag, flat.real], axis=1)
    return np.concatenate([top, low]).astype(np.float32)


def block_copy(field, start, rows, buf, sem):
    return pltpu.make_async_copy(
        field.at[:, pl.ds(start, rows), 0, :], buf.at[:, pl.ds(0, rows), :], sem
    )


def source_block(buf, sums, write):
    for e in range(144):
        sums[e] = buf[e] + buf[144 + e]
    for mt in range(0, 12, 3):
        for nt in range(mt, 12, 3):
            pairs = [(m, n) for m in range(mt, mt + 3) for n in range(nt, nt + 3) if m <= n]
            acc = {}
            for k in range(12):
                rows = sorted({m for m, _ in pairs} | {n for _, n in pairs})
                re = {m: buf[m * 12 + k] for m in rows}
                im = {m: buf[144 + m * 12 + k] for m in rows}
                su = {m: sums[m * 12 + k] for m in rows}
                for m, n in pairs:
                    new = (re[m] * re[n], im[m] * im[n], su[m] * su[n])
                    acc[m, n] = new if k == 0 else tuple(a + b for a, b in zip(acc[m, n], new))
            for m, n in pairs:
                p1, p2, p3 = acc[m, n]
                write(pair_index(m, n), 0.125 * (p1 - p2), 0.125 * (p3 - p1 - p2))


def source_kernel(quarters, sink_ref, field, *refs):
    outs = refs[: len(quarters)]
    bufs, stage, sums, sems, out_sems = refs[len(quarters) :]

    @pl.when(lax.axis_index("ta") == sink_ref[0])
    def _():
        blocks = [(i, half) for i in range(len(quarters)) for half in range(2)]

        def copy_in(number):
            i, half = blocks[number]
            start = (A_START, B_START)[half][quarters[i]]
            return block_copy(field, start, 8 - 2 * half, bufs.at[number], sems.at[number])

        def copy_out(i):
            return pltpu.make_async_copy(stage.at[i], outs[i], out_sems.at[i])

        copy_in(0).start()
        copy_in(1).start()
        for number, (i, half) in enumerate(blocks):
            copy_in(number).wait()
            if number + 2 < len(blocks):
                copy_in(number + 2).start()

            def write(u, re, im, i=i, half=half):
                rows = 8 - 2 * half
                for e, v in ((u, re), (78 + u, im)):
                    first = 320 * half + e % 39 * rows
                    stage[i, e // 39, first : first + rows, :] = v[:rows]

            source_block(bufs.at[number], sums, write)
            if half == 1:
                copy_out(i).start()
        for i in range(len(quarters)):
            copy_out(i).wait()


def source(quarters, sink_time, field):
    count = len(quarters)

    def kernel(*refs):
        source_kernel(quarters, *refs)

    anywhere = pl.BlockSpec(memory_space=pl.ANY)
    return pl.pallas_call(
        kernel,
        in_specs=[pl.BlockSpec(memory_space=pltpu.SMEM), anywhere],
        out_specs=[anywhere] * count,
        out_shape=[jax.ShapeDtypeStruct((4, GROUP, 128), F32)] * count,
        scratch_shapes=[
            pltpu.VMEM((2 * count, 288, 8, 128), F32),
            pltpu.VMEM((count, 4, GROUP, 128), F32),
            pltpu.VMEM((144, 8, 128), F32),
            pltpu.SemaphoreType.DMA((2 * count,)),
            pltpu.SemaphoreType.DMA((count,)),
        ],
        name=f"sink_source_{quarters[0]}",
    )(sink_time, field)


STRIDE = {"y": 16, "x": 4, "z": 1}
AXES = ((("x", 1), ("y", 1), ("z", 1)), (("y", -1), ("z", -1), ("x", -1)))
UNIT = ((1, 0, 0), (0, 1, 0), (0, 0, 1))
TWICE = ((2, 0, 0), (0, 2, 0), (0, 0, 2))
DIAGONAL = ((1, 1, 1), (2, 2, 2), (3, 3, 3))


def moved(vector):
    pairs = []
    for place in range(64):
        for core in range(2):
            target = place
            for (axis, sign), step in zip(AXES[core], vector):
                digit = place // STRIDE[axis] % 4
                target += ((digit + sign * step) % 4 - digit) * STRIDE[axis]
            pairs.append((2 * place + core, 2 * target + core))
    return pairs


def shift(value, vector):
    return lax.ppermute(value, ("ta", "gz"), moved(vector))


def relative(there):
    here, core = lax.axis_index("ta"), lax.axis_index("gz")
    digits = {"y": 4, "x": 2, "z": 0}
    steps = {a: (here >> n) - (there >> n) for a, n in digits.items()}
    out = []
    for i in range(3):
        (a0, s0), (a1, s1) = AXES[0][i], AXES[1][i]
        out.append(jnp.where(core == 0, s0 * steps[a0], s1 * steps[a1]) & 3)
    return out


def labels_at(u, v, w):
    low, high = (u ^ w) & 1, (v ^ w) & 1
    c = low + 2 * high
    hu = (u - (low & (1 - high))) & 3
    hv = (v - (high & (1 - low))) & 3
    hw = (w - (low & high)) & 3
    d_low, d_high = (hu >> 1) ^ (hw >> 1), (hv >> 1) ^ (hw >> 1)
    copy = (hu - 2 * (d_low & (1 - d_high))) & 3
    return c, d_low + 2 * d_high, copy


def received(there, k):
    u, v, w = relative(there)
    du, dv, dw = (0, 0, 0) if k == 0 else UNIT[k - 1]
    c, d, _ = labels_at((u - du) & 3, (v - dv) & 3, (w - dw) & 3)
    return c, d


def pick(index, sources):
    value = sources[-1]
    for i in range(len(sources) - 2, -1, -1):
        value = jnp.where(index == i, sources[i], value)
    return value


def spread(quarters, there, ready):
    c, d, copy = labels_at(*relative(there))
    arrived = [quarters[0]] + [shift(quarters[k], UNIT[k - 1]) for k in (1, 2, 3)]
    c, ready = lax.optimization_barrier((c, ready))
    groups = [pick(c, [a[g] for a in arrived]) for g in range(4)]
    got = [shift(groups[k], TWICE[k - 1]) for k in (1, 2, 3)]
    piece = pick(d, [groups[0]] + got)
    got = [shift(piece, DIAGONAL[k - 1]) for k in (1, 2, 3)]
    piece = pick(copy, [piece] + got)
    own = jnp.stack([piece] + [shift(piece, TWICE[k - 1]) for k in (1, 2, 3)])
    return [own] + [shift(own, UNIT[k]) for k in range(3)], ready


def contract_block(rows, b, slots, s_buf, h_buf, g_buf, sig, s_sum, h_sum, macc, mout):
    for u in range(78):
        part = []
        for e in (u, 78 + u):
            v = g_buf[b, slots[e // 39], e % 39 * rows : e % 39 * rows + rows, :]
            sig[(e // 78) * 78 + u, 0:rows, :] = v
            part.append(v)
        sig[156 + u, 0:rows, :] = part[0] + part[1]
    for e in range(144):
        s_sum[e] = s_buf[b, e] + s_buf[b, 144 + e]
        h_sum[e] = h_buf[b, e] + h_buf[b, 144 + e]

    def spin(alpha, carry):
        base = alpha * 36
        for nt in range(0, 12, 3):
            acc = {}
            for m in range(12):
                h = [
                    (h_buf[b, base + a * 12 + m], h_buf[b, base + (144 + a * 12 + m)], h_sum[base + a * 12 + m])
                    for a in range(3)
                ]
                for n in range(nt, nt + 3):
                    u = pair_index(m, n)
                    g = (sig[u], sig[78 + u], sig[156 + u])
                    for a in range(3):
                        new = tuple(x * y for x, y in zip(h[a], g))
                        acc[a, n] = new if m == 0 else tuple(x + y for x, y in zip(acc[a, n], new))
            conj = {}
            for key, (p1, p2, p3) in acc.items():
                u_, w_ = p1 - p2, p1 + p2 - p3
                conj[key] = (u_, w_, u_ + w_)
            for beta in range(4):
                q = None
                for (a, n), t in conj.items():
                    e = (3 * beta + a) * 12 + n
                    s = (s_buf[b, e], s_buf[b, 144 + e], s_sum[e])
                    new = tuple(x * y for x, y in zip(s, t))
                    q = new if q is None else tuple(x + y for x, y in zip(q, new))
                if nt > 0:
                    q = tuple(q[i] + macc[beta, i] for i in range(3))
                if nt < 9:
                    for i in range(3):
                        macc[beta, i] = q[i]
                else:
                    mout[alpha * 4 + beta] = q[0] - q[1]
                    mout[16 + alpha * 4 + beta] = q[2] - q[0] - q[1]
        return carry

    lax.fori_loop(0, 4, spin, 0)


def project(rows, mout, phases, total):
    for pair in range(rows // 2):
        wide = jnp.concatenate([mout[:, 2 * pair, :], mout[:, 2 * pair + 1, :]], axis=1)
        high = wide.astype(BF16)
        low = (wide - high.astype(F32)).astype(BF16)
        total += lax.dot_general(
            jnp.concatenate([high, low], axis=0),
            phases[pair],
            (((1,), (1,)), ((), ())),
            preferred_element_type=F32,
        )
    return total


def currents(weights, total):
    total = total[:32] + total[32:]
    total = total[:, :64] + total[:, 64:]
    cosine, sine = total[:, :28], total[:, 32:60]
    re = cosine[:16] - sine[16:]
    im = sine[:16] + cosine[16:]
    result = jnp.dot(
        weights,
        jnp.concatenate([re, im], axis=0),
        precision=lax.Precision.HIGHEST,
        preferred_element_type=F32,
    )
    return tuple(result[8 * i : 8 * i + 8] for i in range(4))


def contract_kernel(first, nf, last, sink_ref, prop, back, phases_a, phases_b, *refs):
    fields, refs = refs[:nf], refs[nf:]
    if last:
        before, weights, gammas, keep_ref, send_ref = refs[:5]
        refs = refs[5:]
    else:
        out_ref, refs = refs[0], refs[1:]
    s_buf, h_buf, g_buf, p_buf, sig, s_sum, h_sum, macc, mout, acc, numbers, sems = refs
    nb = 2 * nf
    for i in range(nf):
        numbers[i, 0], numbers[i, 1] = received(sink_ref[0], first + i)

    def first_row(starts, b):
        q = numbers[b % nf, 0]
        start = jnp.int32(starts[3])
        for i in range(3):
            start = jnp.where(q == i, starts[i], start)
        return start

    def copies(b):
        half = b // nf
        rows, lo = (8, 0) if half == 0 else (6, 320)
        starts, phases = ((A_START, phases_a), (B_START, phases_b))[half]
        start = first_row(starts, b)
        return [
            pltpu.make_async_copy(
                fields[b % nf].at[:, pl.ds(lo, 40 * rows), :],
                g_buf.at[b, :, pl.ds(0, 40 * rows), :],
                sems.at[b, 0],
            ),
            block_copy(back, start, rows, h_buf.at[b], sems.at[b, 1]),
            block_copy(prop, start, rows, s_buf.at[b], sems.at[b, 2]),
            pltpu.make_async_copy(
                phases.at[numbers[b % nf, 0]], p_buf.at[b, pl.ds(0, rows // 2)], sems.at[b, 3]
            ),
        ]

    def on(b, action):
        for i in range(nb):

            @pl.when(b == i)
            def _():
                for copy in copies(i):
                    action(copy)

    for copy in copies(0):
        copy.start()
    acc[...] = before[...] if last else jnp.zeros_like(acc)
    for half, rows in ((0, 8), (1, 6)):

        def block(i, carry, half=half, rows=rows):
            b = half * nf + i
            on(b, lambda copy: copy.wait())
            on(b + 1, lambda copy: copy.start())
            slots = [numbers[i, 1] ^ g for g in range(4)]
            contract_block(rows, b, slots, s_buf, h_buf, g_buf, sig, s_sum, h_sum, macc, mout)
            acc[...] = project(rows, mout, p_buf.at[b], acc[...])
            return carry

        lax.fori_loop(0, nf, block, 0)
    if last:
        mout[0, :, :28], mout[1, :, :28], mout[2, :, :28], mout[3, :, :28] = currents(weights[...], acc[...])
        core = lax.axis_index("gz")
        for i in range(16):
            out = (keep_ref, send_ref)[i // 8]
            row = gammas[(i + 8 * core) & 15]
            for part in range(2):
                out[part, pl.ds(i % 8, 1), :] = mout[2 * part + (row >> 3), pl.ds(row & 7, 1), :NP]
    else:
        out_ref[...] = acc[...]


def contract(first, sink_time, prop, back, phases, fields, before=None, weights=None, gammas=None):
    nf = len(fields)
    last = weights is not None

    def kernel(*refs):
        contract_kernel(first, nf, last, *refs)

    anywhere = pl.BlockSpec(memory_space=pl.ANY)
    vmem = pl.BlockSpec(memory_space=pltpu.VMEM)
    smem = pl.BlockSpec(memory_space=pltpu.SMEM)
    if last:
        out_shape = [jax.ShapeDtypeStruct((2, 8, NP), F32)] * 2
    else:
        out_shape = [jax.ShapeDtypeStruct((64, 128), F32)]
    return pl.pallas_call(
        kernel,
        in_specs=[smem] + [anywhere] * (4 + nf) + [vmem, vmem, smem][: 3 * last],
        out_specs=[vmem] * len(out_shape),
        out_shape=out_shape,
        scratch_shapes=[
            pltpu.VMEM((2 * nf, 288, 8, 128), F32),
            pltpu.VMEM((2 * nf, 288, 8, 128), F32),
            pltpu.VMEM((2 * nf, 4, 320, 128), F32),
            pltpu.VMEM((2 * nf, 4, 128, 256), BF16),
            pltpu.VMEM((234, 8, 128), F32),
            pltpu.VMEM((144, 8, 128), F32),
            pltpu.VMEM((144, 8, 128), F32),
            pltpu.VMEM((4, 3, 8, 128), F32),
            pltpu.VMEM((32, 8, 128), F32),
            pltpu.VMEM((64, 128), F32),
            pltpu.SMEM((nf, 2), jnp.int32),
            pltpu.SemaphoreType.DMA((2 * nf, 4)),
        ],
        name=f"contract_{nf}",
    )(sink_time, prop, back, *phases, *fields, *([before, weights, gammas] if last else []))


def cosine_of(wave):
    wave = wave - 24.0 * jnp.floor((wave + 0.5) * (1.0 / 24.0))
    t = (jnp.abs(wave - 12.0) - 6.0) * (math.pi / 12.0)
    t2 = t * t
    value = t2 * (1.0 / 6227020800.0) - 1.0 / 39916800.0
    for k in (362880.0, -5040.0, 120.0, -6.0):
        value = value * t2 + 1.0 / k
    return t + t * (t2 * value)


def site_places():
    out = np.zeros((28, 8, 256), np.float32)
    lane = np.arange(256)
    number = 0
    for starts, pairs in ((A_START, 4), (B_START, 3)):
        for q in range(4):
            for pair in range(pairs):
                site = (starts[q] + 2 * pair) * 128 + lane
                out[number, 0], out[number, 1], out[number, 2] = site // L % L, site % L, site // (L * L)
                out[number, 3] = 0.0 if (pairs, q, pair) == (3, 3, 0) else 1.0
                number += 1
    return out


def phase_kernel(source_ref, momenta, places, out_a, out_b, wide):
    core = lax.axis_index("gz").astype(F32)
    table = momenta[...].astype(F32)
    table = jnp.concatenate([table, jnp.zeros((32 - NP, 3), F32)], axis=0)
    for i in range(3):
        column = jnp.broadcast_to(table[:, i : i + 1], (32, 256))
        wide[i, :32, :] = column
        wide[i, 32:, :] = column
    origin = [source_ref[i].astype(F32) for i in range(3)]
    origin[2] = origin[2] - 12.0 * core
    turn = jnp.where(lax.broadcasted_iota(jnp.int32, (64, 256), 0) < 32, 0.0, 6.0)

    def pair(number, out, q, p):
        wave = turn
        for i in range(3):
            wave = wave + wide[i] * (places[number, i : i + 1, :] - origin[i])
        value = cosine_of(wave) * places[number, 3:4, :]
        high = value.astype(BF16)
        out[q, p, :64, :] = high
        out[q, p, 64:, :] = (value - high.astype(F32)).astype(BF16)

    def step_a(n, carry):
        pair(n, out_a, n >> 2, n & 3)
        return carry

    lax.fori_loop(0, 16, step_a, 0)
    for q in range(4):

        def step_b(p, carry, q=q):
            pair(16 + 3 * q + p, out_b, q, p)
            return carry

        lax.fori_loop(0, 3, step_b, 0)


def phase_blocks(source_position, momenta):
    vmem = pl.BlockSpec(memory_space=pltpu.VMEM)
    return pl.pallas_call(
        phase_kernel,
        in_specs=[pl.BlockSpec(memory_space=pltpu.SMEM), vmem, vmem],
        out_specs=[vmem, vmem],
        out_shape=[
            jax.ShapeDtypeStruct((4, 4, 128, 256), BF16),
            jax.ShapeDtypeStruct((4, 3, 128, 256), BF16),
        ],
        scratch_shapes=[pltpu.VMEM((3, 64, 256), F32)],
        name="phases",
    )(source_position, momenta, jnp.asarray(site_places()))


def body(propagator, backward, sink_time, source_position, momenta, gamma_table):
    prop = propagator.reshape(288, ROWS, 1, 128)
    back = backward.reshape(288, ROWS, 1, 128)
    quarters = dict(zip((1, 2, 3), source((1, 2, 3), sink_time, prop)))
    (quarters[0],) = source((0,), sink_time, prop)
    phases = phase_blocks(source_position, momenta)
    fields, phases = spread(quarters, sink_time[0], phases)
    (own,) = contract(0, sink_time, prop, back, phases, fields[:1])
    keep, send = contract(
        1, sink_time, prop, back, phases, fields[1:], own, jnp.asarray(gamma_weights()), gamma_table
    )
    return (keep + lax.ppermute(send, "gz", [(0, 1), (1, 0)]))[:, None]


def solution(mesh):
    in_specs = (
        P(None, None, None, "ta", "gz"),
        P(None, None, None, "ta", "gz"),
        P(),
        P(),
        P(),
        P(),
    )
    out_specs = P(None, "ta", "gz", None)
    return jax.shard_map(body, mesh=mesh, in_specs=in_specs, out_specs=out_specs, check_vma=False)
```

```python
import math

import jax
import jax.numpy as jnp
import numpy as np
from jax import lax
from jax.experimental import pallas as pl
from jax.experimental.pallas import tpu as pltpu
from jax.sharding import PartitionSpec as P


L = 24
NP = 27
ROWS = 54
A_START = (0, 14, 28, 42)
B_START = (8, 22, 36, 48)
F32 = jnp.float32
BF16 = jnp.bfloat16


def pair_index(m, n):
    m, n = min(m, n), max(m, n)
    return m * 12 - m * (m - 1) // 2 + (n - m)


def gamma_weights():
    paulis = [
        np.eye(2),
        np.array([[0.0, 1.0], [1.0, 0.0]]),
        np.array([[0.0, -1j], [1j, 0.0]]),
        np.array([[1.0, 0.0], [0.0, -1.0]]),
    ]
    matrices = np.stack([np.kron(paulis[number // 4], paulis[number % 4]) for number in range(16)])
    flat = matrices.reshape(16, 16) / (72.0 * math.sqrt(L * L * L))
    top = np.concatenate([flat.real, -flat.imag], axis=1)
    low = np.concatenate([flat.imag, flat.real], axis=1)
    return np.concatenate([top, low]).astype(np.float32)


PIECES = 4


def block_copies(field, start, rows, buf, sems):
    span = 288 // PIECES
    return [
        pltpu.make_async_copy(
            field.at[pl.ds(i * span, span), pl.ds(start, rows), 0, :],
            buf.at[pl.ds(i * span, span), pl.ds(0, rows), :],
            sems.at[i],
        )
        for i in range(PIECES)
    ]


def source_block(buf, sums, write):
    for e in range(144):
        sums[e] = buf[e] + buf[144 + e]
    for mt in range(0, 12, 3):
        for nt in range(mt, 12, 3):
            pairs = [(m, n) for m in range(mt, mt + 3) for n in range(nt, nt + 3) if m <= n]
            acc = {}
            for k in range(12):
                rows = sorted({m for m, _ in pairs} | {n for _, n in pairs})
                re = {m: buf[m * 12 + k] for m in rows}
                im = {m: buf[144 + m * 12 + k] for m in rows}
                su = {m: sums[m * 12 + k] for m in rows}
                for m, n in pairs:
                    new = (re[m] * re[n], im[m] * im[n], su[m] * su[n])
                    acc[m, n] = new if k == 0 else tuple(a + b for a, b in zip(acc[m, n], new))
            for m, n in pairs:
                p1, p2, p3 = acc[m, n]
                write(pair_index(m, n), 0.125 * (p1 - p2), 0.125 * (p3 - p1 - p2))


def source_kernel(blocks, sink_ref, field, *refs):
    outs = refs[: len(blocks)]
    bufs, stage, sums, sems, out_sems = refs[len(blocks) :]

    @pl.when(lax.axis_index("ta") == sink_ref[0])
    def _():
        def copies_in(i):
            quarter, half = blocks[i]
            start = (A_START, B_START)[half][quarter]
            return block_copies(field, start, 8 - 2 * half, bufs.at[i], sems.at[i])

        def copy_out(i):
            rows = 40 * (8 - 2 * blocks[i][1])
            return pltpu.make_async_copy(stage.at[i, :, pl.ds(0, rows), :], outs[i], out_sems.at[i])

        for i in range(min(2, len(blocks))):
            for copy in copies_in(i):
                copy.start()
        for i, (_, half) in enumerate(blocks):
            for copy in copies_in(i):
                copy.wait()
            if i + 2 < len(blocks):
                for copy in copies_in(i + 2):
                    copy.start()

            def write(u, re, im, i=i, rows=8 - 2 * half):
                for e, v in ((u, re), (78 + u, im)):
                    first = e % 39 * rows
                    stage[i, e // 39, first : first + rows, :] = v[:rows]

            source_block(bufs.at[i], sums, write)
            copy_out(i).start()
        for i in range(len(blocks)):
            copy_out(i).wait()


def source(blocks, sink_time, field):
    count = len(blocks)

    def kernel(*refs):
        source_kernel(blocks, *refs)

    anywhere = pl.BlockSpec(memory_space=pl.ANY)
    return pl.pallas_call(
        kernel,
        in_specs=[pl.BlockSpec(memory_space=pltpu.SMEM), anywhere],
        out_specs=[anywhere] * count,
        out_shape=[jax.ShapeDtypeStruct((4, 40 * (8 - 2 * half), 128), F32) for _, half in blocks],
        scratch_shapes=[
            pltpu.VMEM((count, 288, 8, 128), F32),
            pltpu.VMEM((count, 4, 320, 128), F32),
            pltpu.VMEM((144, 8, 128), F32),
            pltpu.SemaphoreType.DMA((count, PIECES)),
            pltpu.SemaphoreType.DMA((count,)),
        ],
    )(sink_time, field)


STRIDE = {"y": 16, "x": 4, "z": 1}
AXES = ((("x", 1), ("y", 1), ("z", 1)), (("y", -1), ("z", -1), ("x", -1)))
UNIT = ((1, 0, 0), (0, 1, 0), (0, 0, 1))
TWICE = ((2, 0, 0), (0, 2, 0), (0, 0, 2))
DIAGONAL = ((1, 1, 1), (2, 2, 2), (3, 3, 3))


def moved(vector):
    pairs = []
    for place in range(64):
        for core in range(2):
            target = place
            for (axis, sign), step in zip(AXES[core], vector):
                digit = place // STRIDE[axis] % 4
                target += ((digit + sign * step) % 4 - digit) * STRIDE[axis]
            pairs.append((2 * place + core, 2 * target + core))
    return pairs


def shift(value, vector):
    return lax.ppermute(value, ("ta", "gz"), moved(vector))


def relative(there):
    here, core = lax.axis_index("ta"), lax.axis_index("gz")
    digits = {"y": 4, "x": 2, "z": 0}
    steps = {a: (here >> n) - (there >> n) for a, n in digits.items()}
    out = []
    for i in range(3):
        (a0, s0), (a1, s1) = AXES[0][i], AXES[1][i]
        out.append(jnp.where(core == 0, s0 * steps[a0], s1 * steps[a1]) & 3)
    return out


def labels_at(u, v, w):
    low, high = (u ^ w) & 1, (v ^ w) & 1
    c = low + 2 * high
    hu = (u - (low & (1 - high))) & 3
    hv = (v - (high & (1 - low))) & 3
    hw = (w - (low & high)) & 3
    d_low, d_high = (hu >> 1) ^ (hw >> 1), (hv >> 1) ^ (hw >> 1)
    copy = (hu - 2 * (d_low & (1 - d_high))) & 3
    return c, d_low + 2 * d_high, copy


def received(there, k):
    u, v, w = relative(there)
    du, dv, dw = (0, 0, 0) if k == 0 else UNIT[k - 1]
    c, d, _ = labels_at((u - du) & 3, (v - dv) & 3, (w - dw) & 3)
    return c, d


def pick(index, sources):
    value = sources[-1]
    for i in range(len(sources) - 2, -1, -1):
        value = jnp.where(index == i, sources[i], value)
    return value


def spread(upper, lower, there, ready):
    c, d, copy = labels_at(*relative(there))
    upper = [upper[0]] + [shift(upper[k], UNIT[k - 1]) for k in (1, 2, 3)]
    lower = [lower[0]] + [shift(lower[k], UNIT[k - 1]) for k in (1, 2, 3)]
    c, ready = lax.optimization_barrier((c, ready))
    groups = [
        jnp.concatenate([pick(c, [a[g] for a in upper]), pick(c, [a[g] for a in lower])])
        for g in range(4)
    ]
    got = [shift(groups[k], TWICE[k - 1]) for k in (1, 2, 3)]
    piece = pick(d, [groups[0]] + got)
    got = [shift(piece, DIAGONAL[k - 1]) for k in (1, 2, 3)]
    piece = pick(copy, [piece] + got)
    groups = [piece] + [shift(piece, TWICE[k - 1]) for k in (1, 2, 3)]
    lower = jnp.stack([g[320:] for g in groups])
    lower_got = [shift(lower, UNIT[k]) for k in range(3)]
    upper = jnp.stack([g[:320] for g in groups])
    upper_got = [shift(upper, UNIT[k]) for k in range(3)]
    return [upper] + upper_got, [lower] + lower_got, ready


def contract_block(rows, b, slots, s_buf, h_buf, g_buf, sig, s_sum, h_sum, macc, mout):
    for u in range(78):
        part = []
        for e in (u, 78 + u):
            v = g_buf[b, slots[e // 39], e % 39 * rows : e % 39 * rows + rows, :]
            sig[(e // 78) * 78 + u, 0:rows, :] = v
            part.append(v)
        sig[156 + u, 0:rows, :] = part[0] + part[1]
    for e in range(144):
        s_sum[e] = s_buf[b, e] + s_buf[b, 144 + e]
        h_sum[e] = h_buf[b, e] + h_buf[b, 144 + e]

    def spin(alpha, carry):
        base = alpha * 36
        for nt in range(0, 12, 3):
            acc = {}
            for m in range(12):
                h = [
                    (h_buf[b, base + a * 12 + m], h_buf[b, base + (144 + a * 12 + m)], h_sum[base + a * 12 + m])
                    for a in range(3)
                ]
                for n in range(nt, nt + 3):
                    u = pair_index(m, n)
                    g = (sig[u], sig[78 + u], sig[156 + u])
                    for a in range(3):
                        new = tuple(x * y for x, y in zip(h[a], g))
                        acc[a, n] = new if m == 0 else tuple(x + y for x, y in zip(acc[a, n], new))
            conj = {}
            for key, (p1, p2, p3) in acc.items():
                u_, w_ = p1 - p2, p1 + p2 - p3
                conj[key] = (u_, w_, u_ + w_)
            for beta in range(4):
                q = None
                for (a, n), t in conj.items():
                    e = (3 * beta + a) * 12 + n
                    s = (s_buf[b, e], s_buf[b, 144 + e], s_sum[e])
                    new = tuple(x * y for x, y in zip(s, t))
                    q = new if q is None else tuple(x + y for x, y in zip(q, new))
                if nt > 0:
                    q = tuple(q[i] + macc[beta, i] for i in range(3))
                if nt < 9:
                    for i in range(3):
                        macc[beta, i] = q[i]
                else:
                    mout[alpha * 4 + beta] = q[0] - q[1]
                    mout[16 + alpha * 4 + beta] = q[2] - q[0] - q[1]
        return carry

    lax.fori_loop(0, 4, spin, 0)


def project(rows, mout, phases, total):
    for pair in range(rows // 2):
        wide = jnp.concatenate([mout[:, 2 * pair, :], mout[:, 2 * pair + 1, :]], axis=1)
        high = wide.astype(BF16)
        low = (wide - high.astype(F32)).astype(BF16)
        total += lax.dot_general(
            jnp.concatenate([high, low], axis=0),
            phases[pair],
            (((1,), (1,)), ((), ())),
            preferred_element_type=F32,
        )
    return total


def currents(weights, total):
    total = total[:32] + total[32:]
    total = total[:, :64] + total[:, 64:]
    cosine, sine = total[:, :28], total[:, 32:60]
    re = cosine[:16] - sine[16:]
    im = sine[:16] + cosine[16:]
    result = jnp.dot(
        weights,
        jnp.concatenate([re, im], axis=0),
        precision=lax.Precision.HIGHEST,
        preferred_element_type=F32,
    )
    return tuple(result[8 * i : 8 * i + 8] for i in range(4))


def contract_kernel(blocks, more, last, sink_ref, prop, back, phases_a, phases_b, *refs):
    nb = len(blocks)
    fields, refs = refs[:nb], refs[nb:]
    if more:
        before, refs = refs[0], refs[1:]
    if last:
        weights, gammas, keep_ref, send_ref = refs[:4]
        refs = refs[4:]
    else:
        out_ref, refs = refs[0], refs[1:]
    s_buf, h_buf, g_buf, p_buf, sig, s_sum, h_sum, macc, mout, acc, numbers, sems = refs

    def copies(b):
        half = blocks[b][1]
        rows = 8 - 2 * half
        starts, phases = ((A_START, phases_a), (B_START, phases_b))[half]
        start = jnp.int32(starts[3])
        for i in range(3):
            start = jnp.where(numbers[b, 0] == i, starts[i], start)
        return [
            pltpu.make_async_copy(
                fields[b], g_buf.at[b, :, pl.ds(0, 40 * rows), :], sems.at[b, 2 * PIECES]
            ),
            *block_copies(back, start, rows, h_buf.at[b], sems.at[b, pl.ds(0, PIECES)]),
            *block_copies(prop, start, rows, s_buf.at[b], sems.at[b, pl.ds(PIECES, PIECES)]),
            pltpu.make_async_copy(
                phases.at[numbers[b, 0]], p_buf.at[b, pl.ds(0, rows // 2)], sems.at[b, 2 * PIECES + 1]
            ),
        ]

    def on(b, action):
        for i in range(nb):

            @pl.when(b == i)
            def _():
                for copy in copies(i):
                    action(copy)

    for b, (k, _) in enumerate(blocks):
        numbers[b, 0], numbers[b, 1] = received(sink_ref[0], k)
    for copy in copies(0):
        copy.start()
    acc[...] = before[...] if more else jnp.zeros_like(acc)
    for half in (0, 1):
        chosen = [b for b in range(nb) if blocks[b][1] == half]
        rows = 8 - 2 * half

        def block(b, carry, rows=rows):
            on(b, lambda copy: copy.wait())
            on(b + 1, lambda copy: copy.start())
            slots = [numbers[b, 1] ^ g for g in range(4)]
            contract_block(rows, b, slots, s_buf, h_buf, g_buf, sig, s_sum, h_sum, macc, mout)
            acc[...] = project(rows, mout, p_buf.at[b], acc[...])
            return carry

        if chosen:
            lax.fori_loop(chosen[0], chosen[-1] + 1, block, 0)
    if last:
        mout[0, :, :28], mout[1, :, :28], mout[2, :, :28], mout[3, :, :28] = currents(weights[...], acc[...])
        core = lax.axis_index("gz")
        for i in range(16):
            out = (keep_ref, send_ref)[i // 8]
            row = gammas[(i + 8 * core) & 15]
            for part in range(2):
                out[part, pl.ds(i % 8, 1), :] = mout[2 * part + (row >> 3), pl.ds(row & 7, 1), :NP]
    else:
        out_ref[...] = acc[...]


def contract(blocks, sink_time, prop, back, phases, fields, before=None, weights=None, gammas=None):
    nb = len(blocks)
    more, last = before is not None, weights is not None

    def kernel(*refs):
        contract_kernel(blocks, more, last, *refs)

    anywhere = pl.BlockSpec(memory_space=pl.ANY)
    vmem = pl.BlockSpec(memory_space=pltpu.VMEM)
    smem = pl.BlockSpec(memory_space=pltpu.SMEM)
    if last:
        out_shape = [jax.ShapeDtypeStruct((2, 8, NP), F32)] * 2
    else:
        out_shape = [jax.ShapeDtypeStruct((64, 128), F32)]
    return pl.pallas_call(
        kernel,
        in_specs=[smem] + [anywhere] * (4 + nb) + [vmem] * more + [vmem, smem] * last,
        out_specs=[vmem] * len(out_shape),
        out_shape=out_shape,
        scratch_shapes=[
            pltpu.VMEM((nb, 288, 8, 128), F32),
            pltpu.VMEM((nb, 288, 8, 128), F32),
            pltpu.VMEM((nb, 4, 320, 128), F32),
            pltpu.VMEM((nb, 4, 128, 256), BF16),
            pltpu.VMEM((234, 8, 128), F32),
            pltpu.VMEM((144, 8, 128), F32),
            pltpu.VMEM((144, 8, 128), F32),
            pltpu.VMEM((4, 3, 8, 128), F32),
            pltpu.VMEM((32, 8, 128), F32),
            pltpu.VMEM((64, 128), F32),
            pltpu.SMEM((nb, 2), jnp.int32),
            pltpu.SemaphoreType.DMA((nb, 2 * PIECES + 2)),
        ],
    )(sink_time, prop, back, *phases, *fields, *([before] if more else []), *([weights, gammas] if last else []))


def cosine_of(wave):
    wave = wave - 24.0 * jnp.floor((wave + 0.5) * (1.0 / 24.0))
    t = (jnp.abs(wave - 12.0) - 6.0) * (math.pi / 12.0)
    t2 = t * t
    value = t2 * (1.0 / 6227020800.0) - 1.0 / 39916800.0
    for k in (362880.0, -5040.0, 120.0, -6.0):
        value = value * t2 + 1.0 / k
    return t + t * (t2 * value)


def site_places():
    out = np.zeros((28, 8, 256), np.float32)
    lane = np.arange(256)
    number = 0
    for starts, pairs in ((A_START, 4), (B_START, 3)):
        for q in range(4):
            for pair in range(pairs):
                site = (starts[q] + 2 * pair) * 128 + lane
                out[number, 0], out[number, 1], out[number, 2] = site // L % L, site % L, site // (L * L)
                out[number, 3] = 0.0 if (pairs, q, pair) == (3, 3, 0) else 1.0
                number += 1
    return out


def phase_kernel(source_ref, momenta, places, out_a, out_b, wide):
    core = lax.axis_index("gz").astype(F32)
    table = momenta[...].astype(F32)
    table = jnp.concatenate([table, jnp.zeros((32 - NP, 3), F32)], axis=0)
    for i in range(3):
        column = jnp.broadcast_to(table[:, i : i + 1], (32, 256))
        wide[i, :32, :] = column
        wide[i, 32:, :] = column
    origin = [source_ref[i].astype(F32) for i in range(3)]
    origin[2] = origin[2] - 12.0 * core
    turn = jnp.where(lax.broadcasted_iota(jnp.int32, (64, 256), 0) < 32, 0.0, 6.0)

    def pair(number, out, q, p):
        wave = turn
        for i in range(3):
            wave = wave + wide[i] * (places[number, i : i + 1, :] - origin[i])
        value = cosine_of(wave) * places[number, 3:4, :]
        high = value.astype(BF16)
        out[q, p, :64, :] = high
        out[q, p, 64:, :] = (value - high.astype(F32)).astype(BF16)

    def step_a(n, carry):
        pair(n, out_a, n >> 2, n & 3)
        return carry

    lax.fori_loop(0, 16, step_a, 0)
    for q in range(4):

        def step_b(p, carry, q=q):
            pair(16 + 3 * q + p, out_b, q, p)
            return carry

        lax.fori_loop(0, 3, step_b, 0)


def phase_blocks(source_position, momenta):
    vmem = pl.BlockSpec(memory_space=pltpu.VMEM)
    return pl.pallas_call(
        phase_kernel,
        in_specs=[pl.BlockSpec(memory_space=pltpu.SMEM), vmem, vmem],
        out_specs=[vmem, vmem],
        out_shape=[
            jax.ShapeDtypeStruct((4, 4, 128, 256), BF16),
            jax.ShapeDtypeStruct((4, 3, 128, 256), BF16),
        ],
        scratch_shapes=[pltpu.VMEM((3, 64, 256), F32)],
        name="phases",
    )(source_position, momenta, jnp.asarray(site_places()))


def body(propagator, backward, sink_time, source_position, momenta, gamma_table):
    prop = propagator.reshape(288, ROWS, 1, 128)
    back = backward.reshape(288, ROWS, 1, 128)
    upper = [None, *source([(1, 0), (2, 0), (3, 0)], sink_time, prop)]
    lower = [None, *source([(1, 1), (2, 1), (3, 1)], sink_time, prop)]
    upper[0], lower[0] = source([(0, 0), (0, 1)], sink_time, prop)
    phases = phase_blocks(source_position, momenta)
    upper, lower, phases = spread(upper, lower, sink_time[0], phases)
    args = (sink_time, prop, back, phases)
    (sums,) = contract([(0, 0), (0, 1)], *args, [upper[0], lower[0]])
    (sums,) = contract([(k, 1) for k in (1, 2, 3)], *args, lower[1:], sums)
    keep, send = contract(
        [(k, 0) for k in (1, 2, 3)], *args, upper[1:], sums, jnp.asarray(gamma_weights()), gamma_table
    )
    return (keep + lax.ppermute(send, "gz", [(0, 1), (1, 0)]))[:, None]


def solution(mesh):
    in_specs = (
        P(None, None, None, "ta", "gz"),
        P(None, None, None, "ta", "gz"),
        P(),
        P(),
        P(),
        P(),
    )
    out_specs = P(None, "ta", "gz", None)
    return jax.shard_map(body, mesh=mesh, in_specs=in_specs, out_specs=out_specs, check_vma=False)
```

```python
import math

import jax
import jax.numpy as jnp
import numpy as np
from jax import lax
from jax.experimental import pallas as pl
from jax.experimental.pallas import tpu as pltpu
from jax.sharding import PartitionSpec as P


L = 24
NP = 27
ROWS = 54
A_START = (0, 14, 28, 42)
B_START = (8, 22, 36, 48)
F32 = jnp.float32
BF16 = jnp.bfloat16


def pair_index(m, n):
    m, n = min(m, n), max(m, n)
    return m * 12 - m * (m - 1) // 2 + (n - m)


def gamma_weights():
    paulis = [
        np.eye(2),
        np.array([[0.0, 1.0], [1.0, 0.0]]),
        np.array([[0.0, -1j], [1j, 0.0]]),
        np.array([[1.0, 0.0], [0.0, -1.0]]),
    ]
    matrices = np.stack([np.kron(paulis[number // 4], paulis[number % 4]) for number in range(16)])
    flat = matrices.reshape(16, 16) / (72.0 * math.sqrt(L * L * L))
    top = np.concatenate([flat.real, -flat.imag], axis=1)
    low = np.concatenate([flat.imag, flat.real], axis=1)
    return np.concatenate([top, low]).astype(np.float32)


def block_copy(field, start, rows, buf, row, sem):
    return pltpu.make_async_copy(
        field.at[:, pl.ds(start, rows), 0, :], buf.at[:, pl.ds(row, rows), :], sem
    )


def source_block(buf, sums, write):
    for e in range(144):
        sums[e] = buf[e] + buf[144 + e]
    for mt in range(0, 12, 3):
        for nt in range(mt, 12, 3):
            pairs = [(m, n) for m in range(mt, mt + 3) for n in range(nt, nt + 3) if m <= n]
            acc = {}
            for k in range(12):
                rows = sorted({m for m, _ in pairs} | {n for _, n in pairs})
                re = {m: buf[m * 12 + k] for m in rows}
                im = {m: buf[144 + m * 12 + k] for m in rows}
                su = {m: sums[m * 12 + k] for m in rows}
                for m, n in pairs:
                    new = (re[m] * re[n], im[m] * im[n], su[m] * su[n])
                    acc[m, n] = new if k == 0 else tuple(a + b for a, b in zip(acc[m, n], new))
            for m, n in pairs:
                p1, p2, p3 = acc[m, n]
                write(pair_index(m, n), 0.125 * (p1 - p2), 0.125 * (p3 - p1 - p2))


def source_kernel(blocks, sink_ref, field, *refs):
    outs = refs[: len(blocks)]
    bufs, stage, sums, sems, out_sems = refs[len(blocks) :]

    @pl.when(lax.axis_index("ta") == sink_ref[0])
    def _():
        def copy_in(i):
            quarter, half = blocks[i]
            start = (A_START, B_START)[half][quarter]
            return block_copy(field, start, 8 - 2 * half, bufs.at[i], 0, sems.at[i])

        def copy_out(i):
            rows = 40 * (8 - 2 * blocks[i][1])
            return pltpu.make_async_copy(stage.at[i, :, pl.ds(0, rows), :], outs[i], out_sems.at[i])

        for i in range(min(2, len(blocks))):
            copy_in(i).start()
        for i, (_, half) in enumerate(blocks):
            copy_in(i).wait()
            if i + 2 < len(blocks):
                copy_in(i + 2).start()

            def write(u, re, im, i=i, rows=8 - 2 * half):
                for e, v in ((u, re), (78 + u, im)):
                    first = e % 39 * rows
                    stage[i, e // 39, first : first + rows, :] = v[:rows]

            source_block(bufs.at[i], sums, write)
            copy_out(i).start()
        for i in range(len(blocks)):
            copy_out(i).wait()


def source(blocks, sink_time, field):
    count = len(blocks)

    def kernel(*refs):
        source_kernel(blocks, *refs)

    anywhere = pl.BlockSpec(memory_space=pl.ANY)
    return pl.pallas_call(
        kernel,
        in_specs=[pl.BlockSpec(memory_space=pltpu.SMEM), anywhere],
        out_specs=[anywhere] * count,
        out_shape=[jax.ShapeDtypeStruct((4, 40 * (8 - 2 * half), 128), F32) for _, half in blocks],
        scratch_shapes=[
            pltpu.VMEM((count, 288, 8, 128), F32),
            pltpu.VMEM((count, 4, 320, 128), F32),
            pltpu.VMEM((144, 8, 128), F32),
            pltpu.SemaphoreType.DMA((count,)),
            pltpu.SemaphoreType.DMA((count,)),
        ],
    )(sink_time, field)


STRIDE = {"y": 16, "x": 4, "z": 1}
AXES = ((("x", 1), ("y", 1), ("z", 1)), (("y", -1), ("z", -1), ("x", -1)))
UNIT = ((1, 0, 0), (0, 1, 0), (0, 0, 1))
TWICE = ((2, 0, 0), (0, 2, 0), (0, 0, 2))
DIAGONAL = ((1, 1, 1), (2, 2, 2), (3, 3, 3))


def moved(vector):
    pairs = []
    for place in range(64):
        for core in range(2):
            target = place
            for (axis, sign), step in zip(AXES[core], vector):
                digit = place // STRIDE[axis] % 4
                target += ((digit + sign * step) % 4 - digit) * STRIDE[axis]
            pairs.append((2 * place + core, 2 * target + core))
    return pairs


def shift(value, vector):
    return lax.ppermute(value, ("ta", "gz"), moved(vector))


def relative(there):
    here, core = lax.axis_index("ta"), lax.axis_index("gz")
    digits = {"y": 4, "x": 2, "z": 0}
    steps = {a: (here >> n) - (there >> n) for a, n in digits.items()}
    out = []
    for i in range(3):
        (a0, s0), (a1, s1) = AXES[0][i], AXES[1][i]
        out.append(jnp.where(core == 0, s0 * steps[a0], s1 * steps[a1]) & 3)
    return out


def labels_at(u, v, w):
    low, high = (u ^ w) & 1, (v ^ w) & 1
    c = low + 2 * high
    hu = (u - (low & (1 - high))) & 3
    hv = (v - (high & (1 - low))) & 3
    hw = (w - (low & high)) & 3
    d_low, d_high = (hu >> 1) ^ (hw >> 1), (hv >> 1) ^ (hw >> 1)
    copy = (hu - 2 * (d_low & (1 - d_high))) & 3
    return c, d_low + 2 * d_high, copy


def received(there, k):
    u, v, w = relative(there)
    du, dv, dw = (0, 0, 0) if k == 0 else UNIT[k - 1]
    c, d, _ = labels_at((u - du) & 3, (v - dv) & 3, (w - dw) & 3)
    return c, d


def pick(index, sources):
    value = sources[-1]
    for i in range(len(sources) - 2, -1, -1):
        value = jnp.where(index == i, sources[i], value)
    return value


def spread(upper, lower, there, ready):
    c, d, copy = labels_at(*relative(there))
    upper = [upper[0]] + [shift(upper[k], UNIT[k - 1]) for k in (1, 2, 3)]
    lower = [lower[0]] + [shift(lower[k], UNIT[k - 1]) for k in (1, 2, 3)]
    c, ready = lax.optimization_barrier((c, ready))
    groups = [
        jnp.concatenate([pick(c, [a[g] for a in upper]), pick(c, [a[g] for a in lower])])
        for g in range(4)
    ]
    got = [shift(groups[k], TWICE[k - 1]) for k in (1, 2, 3)]
    piece = pick(d, [groups[0]] + got)
    got = [shift(piece, DIAGONAL[k - 1]) for k in (1, 2, 3)]
    piece = pick(copy, [piece] + got)
    groups = [piece] + [shift(piece, TWICE[k - 1]) for k in (1, 2, 3)]
    lower = jnp.stack([g[320:] for g in groups])
    lower_got = [shift(lower, UNIT[k]) for k in range(3)]
    upper = jnp.stack([g[:320] for g in groups])
    upper_got = [shift(upper, UNIT[k]) for k in range(3)]
    return [upper] + upper_got, [lower] + lower_got, ready


def unpack(b, parts, slots, g_buf, sig):
    for u in range(78):
        for f, row, skip, count, rows in parts:
            both = []
            for e in (u, 78 + u):
                first = e % 39 * rows + skip
                v = g_buf[f, slots[f][e // 39], first : first + count, :]
                sig[b, e, row : row + count, :] = v
                both.append(v)
            sig[b, 156 + u, row : row + count, :] = both[0] + both[1]


def contract_block(b, s_buf, h_buf, sig, s_sum, h_sum, macc, mout):
    for e in range(144):
        s_sum[e] = s_buf[b, e] + s_buf[b, 144 + e]
        h_sum[e] = h_buf[b, e] + h_buf[b, 144 + e]

    def spin(alpha, carry):
        base = alpha * 36
        for nt in range(0, 12, 3):
            acc = {}
            for m in range(12):
                h = [
                    (h_buf[b, base + a * 12 + m], h_buf[b, base + (144 + a * 12 + m)], h_sum[base + a * 12 + m])
                    for a in range(3)
                ]
                for n in range(nt, nt + 3):
                    u = pair_index(m, n)
                    g = (sig[b, u], sig[b, 78 + u], sig[b, 156 + u])
                    for a in range(3):
                        new = tuple(x * y for x, y in zip(h[a], g))
                        acc[a, n] = new if m == 0 else tuple(x + y for x, y in zip(acc[a, n], new))
            conj = {}
            for key, (p1, p2, p3) in acc.items():
                u_, w_ = p1 - p2, p1 + p2 - p3
                conj[key] = (u_, w_, u_ + w_)
            for beta in range(4):
                q = None
                for (a, n), t in conj.items():
                    e = (3 * beta + a) * 12 + n
                    s = (s_buf[b, e], s_buf[b, 144 + e], s_sum[e])
                    new = tuple(x * y for x, y in zip(s, t))
                    q = new if q is None else tuple(x + y for x, y in zip(q, new))
                if nt > 0:
                    q = tuple(q[i] + macc[beta, i] for i in range(3))
                if nt < 9:
                    for i in range(3):
                        macc[beta, i] = q[i]
                else:
                    mout[alpha * 4 + beta] = q[0] - q[1]
                    mout[16 + alpha * 4 + beta] = q[2] - q[0] - q[1]
        return carry

    lax.fori_loop(0, 4, spin, 0)


def project(mout, phases, total):
    for pair in range(4):
        wide = jnp.concatenate([mout[:, 2 * pair, :], mout[:, 2 * pair + 1, :]], axis=1)
        high = wide.astype(BF16)
        low = (wide - high.astype(F32)).astype(BF16)
        total += lax.dot_general(
            jnp.concatenate([high, low], axis=0),
            phases[pair],
            (((1,), (1,)), ((), ())),
            preferred_element_type=F32,
        )
    return total


def currents(weights, total):
    total = total[:32] + total[32:]
    total = total[:, :64] + total[:, 64:]
    cosine, sine = total[:, :28], total[:, 32:60]
    re = cosine[:16] - sine[16:]
    im = sine[:16] + cosine[16:]
    result = jnp.dot(
        weights,
        jnp.concatenate([re, im], axis=0),
        precision=lax.Precision.HIGHEST,
        preferred_element_type=F32,
    )
    return tuple(result[8 * i : 8 * i + 8] for i in range(4))


def contract_kernel(half, numbered, more, last, sink_ref, prop, back, phases, *refs):
    rows = 8 - 2 * half
    nf = len(numbered)
    nb = nf * rows // 8
    fields, refs = refs[:nf], refs[nf:]
    if more:
        before, refs = refs[0], refs[1:]
    if last:
        weights, gammas, keep_ref, send_ref = refs[:4]
        refs = refs[4:]
    else:
        out_ref, refs = refs[0], refs[1:]
    s_buf, h_buf, g_buf, p_buf, sig, s_sum, h_sum, macc, mout, acc, numbers, sems, g_sems = refs
    parts = []
    for b in range(nb):
        parts.append([])
        row = 0
        while row < 8:
            f, skip = divmod(8 * b + row, rows)
            count = min(rows - skip, 8 - row)
            parts[b].append((f, row, skip, count, rows))
            row += count
    opens = [sorted({p[0] for p in parts[b]} - {p[0] for q in parts[:b] for p in q}) for b in range(nb)]

    def copies(b):
        out = [pltpu.make_async_copy(fields[f], g_buf.at[f], g_sems.at[f]) for f in opens[b]]
        for i, (f, row, skip, count, _) in enumerate(parts[b]):
            starts = (A_START, B_START)[half]
            start = jnp.int32(starts[3])
            for q in range(3):
                start = jnp.where(numbers[f, 0] == q, starts[q], start)
            out += [
                block_copy(back, start + skip, count, h_buf.at[b], row, sems.at[b, i, 0]),
                block_copy(prop, start + skip, count, s_buf.at[b], row, sems.at[b, i, 1]),
                pltpu.make_async_copy(
                    phases.at[numbers[f, 0], pl.ds(skip // 2, count // 2)],
                    p_buf.at[b, pl.ds(row // 2, count // 2)],
                    sems.at[b, i, 2],
                ),
            ]
        return out

    for f, k in enumerate(numbered):
        numbers[f, 0], numbers[f, 1] = received(sink_ref[0], k)
    for copy in copies(0):
        copy.start()
    acc[...] = before[...] if more else jnp.zeros_like(acc)

    def block(b, carry):
        for i in range(nb):

            @pl.when(b == i)
            def _():
                for copy in copies(i):
                    copy.wait()
                if i + 1 < nb:
                    for copy in copies(i + 1):
                        copy.start()
                slots = {p[0]: [numbers[p[0], 1] ^ g for g in range(4)] for p in parts[i]}
                unpack(i, parts[i], slots, g_buf, sig)

        contract_block(b, s_buf, h_buf, sig, s_sum, h_sum, macc, mout)
        acc[...] = project(mout, p_buf.at[b], acc[...])
        return carry

    lax.fori_loop(0, nb, block, 0)
    if last:
        mout[0, :, :28], mout[1, :, :28], mout[2, :, :28], mout[3, :, :28] = currents(weights[...], acc[...])
        core = lax.axis_index("gz")
        for i in range(16):
            out = (keep_ref, send_ref)[i // 8]
            row = gammas[(i + 8 * core) & 15]
            for part in range(2):
                out[part, pl.ds(i % 8, 1), :] = mout[2 * part + (row >> 3), pl.ds(row & 7, 1), :NP]
    else:
        out_ref[...] = acc[...]


def contract(half, numbered, sink_time, prop, back, phases, fields, before=None, weights=None, gammas=None):
    nf = len(numbered)
    rows = 8 - 2 * half
    nb = nf * rows // 8
    more, last = before is not None, weights is not None

    def kernel(*refs):
        contract_kernel(half, numbered, more, last, *refs)

    anywhere = pl.BlockSpec(memory_space=pl.ANY)
    vmem = pl.BlockSpec(memory_space=pltpu.VMEM)
    smem = pl.BlockSpec(memory_space=pltpu.SMEM)
    if last:
        out_shape = [jax.ShapeDtypeStruct((2, 8, NP), F32)] * 2
    else:
        out_shape = [jax.ShapeDtypeStruct((64, 128), F32)]
    return pl.pallas_call(
        kernel,
        in_specs=[smem] + [anywhere] * (3 + nf) + [vmem] * more + [vmem, smem] * last,
        out_specs=[vmem] * len(out_shape),
        out_shape=out_shape,
        scratch_shapes=[
            pltpu.VMEM((nb, 288, 8, 128), F32),
            pltpu.VMEM((nb, 288, 8, 128), F32),
            pltpu.VMEM((nf, 4, 40 * rows, 128), F32),
            pltpu.VMEM((nb, 4, 128, 256), BF16),
            pltpu.VMEM((nb, 234, 8, 128), F32),
            pltpu.VMEM((144, 8, 128), F32),
            pltpu.VMEM((144, 8, 128), F32),
            pltpu.VMEM((4, 3, 8, 128), F32),
            pltpu.VMEM((32, 8, 128), F32),
            pltpu.VMEM((64, 128), F32),
            pltpu.SMEM((nf, 2), jnp.int32),
            pltpu.SemaphoreType.DMA((nb, 2, 3)),
            pltpu.SemaphoreType.DMA((nf,)),
        ],
    )(sink_time, prop, back, phases, *fields, *([before] if more else []), *([weights, gammas] if last else []))


def cosine_of(wave):
    wave = wave - 24.0 * jnp.floor((wave + 0.5) * (1.0 / 24.0))
    t = (jnp.abs(wave - 12.0) - 6.0) * (math.pi / 12.0)
    t2 = t * t
    value = t2 * (1.0 / 6227020800.0) - 1.0 / 39916800.0
    for k in (362880.0, -5040.0, 120.0, -6.0):
        value = value * t2 + 1.0 / k
    return t + t * (t2 * value)


def site_places():
    out = np.zeros((28, 8, 256), np.float32)
    lane = np.arange(256)
    number = 0
    for starts, pairs in ((A_START, 4), (B_START, 3)):
        for q in range(4):
            for pair in range(pairs):
                site = (starts[q] + 2 * pair) * 128 + lane
                out[number, 0], out[number, 1], out[number, 2] = site // L % L, site % L, site // (L * L)
                out[number, 3] = 0.0 if (pairs, q, pair) == (3, 3, 0) else 1.0
                number += 1
    return out


def phase_kernel(source_ref, momenta, places, out_a, out_b, wide):
    core = lax.axis_index("gz").astype(F32)
    table = momenta[...].astype(F32)
    table = jnp.concatenate([table, jnp.zeros((32 - NP, 3), F32)], axis=0)
    for i in range(3):
        column = jnp.broadcast_to(table[:, i : i + 1], (32, 256))
        wide[i, :32, :] = column
        wide[i, 32:, :] = column
    origin = [source_ref[i].astype(F32) for i in range(3)]
    origin[2] = origin[2] - 12.0 * core
    turn = jnp.where(lax.broadcasted_iota(jnp.int32, (64, 256), 0) < 32, 0.0, 6.0)

    def pair(number, out, q, p):
        wave = turn
        for i in range(3):
            wave = wave + wide[i] * (places[number, i : i + 1, :] - origin[i])
        value = cosine_of(wave) * places[number, 3:4, :]
        high = value.astype(BF16)
        out[q, p, :64, :] = high
        out[q, p, 64:, :] = (value - high.astype(F32)).astype(BF16)

    def step_a(n, carry):
        pair(n, out_a, n >> 2, n & 3)
        return carry

    lax.fori_loop(0, 16, step_a, 0)
    for q in range(4):

        def step_b(p, carry, q=q):
            pair(16 + 3 * q + p, out_b, q, p)
            return carry

        lax.fori_loop(0, 3, step_b, 0)


def phase_blocks(source_position, momenta):
    vmem = pl.BlockSpec(memory_space=pltpu.VMEM)
    return pl.pallas_call(
        phase_kernel,
        in_specs=[pl.BlockSpec(memory_space=pltpu.SMEM), vmem, vmem],
        out_specs=[vmem, vmem],
        out_shape=[
            jax.ShapeDtypeStruct((4, 4, 128, 256), BF16),
            jax.ShapeDtypeStruct((4, 3, 128, 256), BF16),
        ],
        scratch_shapes=[pltpu.VMEM((3, 64, 256), F32)],
        name="phases",
    )(source_position, momenta, jnp.asarray(site_places()))


def body(propagator, backward, sink_time, source_position, momenta, gamma_table):
    prop = propagator.reshape(288, ROWS, 1, 128)
    back = backward.reshape(288, ROWS, 1, 128)
    upper = [None, *source([(1, 0), (2, 0), (3, 0)], sink_time, prop)]
    lower = [None, *source([(1, 1), (2, 1), (3, 1)], sink_time, prop)]
    upper[0], lower[0] = source([(0, 0), (0, 1)], sink_time, prop)
    phases = phase_blocks(source_position, momenta)
    upper, lower, phases = spread(upper, lower, sink_time[0], phases)
    (sums,) = contract(0, (0,), sink_time, prop, back, phases[0], upper[:1])
    (sums,) = contract(1, (0, 1, 2, 3), sink_time, prop, back, phases[1], lower, sums)
    keep, send = contract(
        0, (1, 2, 3), sink_time, prop, back, phases[0], upper[1:], sums, jnp.asarray(gamma_weights()), gamma_table
    )
    return (keep + lax.ppermute(send, "gz", [(0, 1), (1, 0)]))[:, None]


def solution(mesh):
    in_specs = (
        P(None, None, None, "ta", "gz"),
        P(None, None, None, "ta", "gz"),
        P(),
        P(),
        P(),
        P(),
    )
    out_specs = P(None, "ta", "gz", None)
    return jax.shard_map(body, mesh=mesh, in_specs=in_specs, out_specs=out_specs, check_vma=False)
```
